256 devices in a mesh: tmpl: 32 (over x, y, core), grid: 8 (over z).
Axes of the slice: x: 4, y: 4, z: 8, core: 2. Of those that a mesh axis runs over, the one named last changes fastest.
Arguments:
- spectrum: float32 [1024, 64, 64, 128], P('tmpl', 'grid'), may hold values from -12 to 12
Outputs:
- best_scores: float32 [4, 64, 64, 64], P(None, 'grid', 'tmpl')
- coherence: float32 [64, 64, 64], P('grid', 'tmpl')
The draws below stay inside these ranges and needn't reach their ends.
All inputs are finite; a program needn't handle non-finite values.
Results may differ from the reference program's by a relative error of at most 0.0001.
Values sent between devices are 32-bit elements; how exact they have to be, the bound alone decides.
No kernel may reach another device: no remote copies, remote signals or barrier semaphores. Data moves between devices by JAX's collectives and lax.ppermute only.
A program may use at most 128 MiB of HBM per device.

```python
import math
import jax
import jax.numpy as jnp
from jax import lax

NG = 64
TEMPLATES = 1024
TOP = 4


def log_uniform(key, shape, low, high):
    return jnp.exp(jax.random.uniform(key, shape, jnp.float32, math.log(low), math.log(high)))


def draw_spectrum(key, part):
    streams = jax.random.split(jax.random.fold_in(key, 11), 8)
    shape = (TEMPLATES, NG, NG, 2 * NG)
    base = jnp.clip(0.125 * jax.random.normal(streams[0], shape, jnp.float32), -0.75, 0.75)
    factor = log_uniform(streams[1], (TEMPLATES, NG, 1, 1), 0.5, 2.0)
    offset = jax.random.normal(streams[3], (TEMPLATES, NG), jnp.float32)
    values = base * factor
    values = values.at[:, :, :, 0].add(offset[:, :, None])
    return jnp.clip(values, -12.0, 12.0)


def setup_inputs(seed: int = 0) -> dict:
    streams_of = jax.random.split(jax.random.key(seed), 2)
    spectrum = draw_spectrum(jax.random.fold_in(streams_of[1], 71), 0)
    return dict(spectrum=spectrum)


FLOOR = -1e+30
SPREAD_FLOOR = 0.25

def phase_table(length):
    order = jnp.arange(length, dtype=jnp.int32)
    turns = order[:, None] * order[None, :] % length
    angle = turns.astype(jnp.float32) * (2.0 * math.pi / length)
    return jnp.concatenate([jnp.cos(angle), -jnp.sin(angle)], axis=0)

def merge_top(former, latter):
    result = []
    for rank_out in range(len(former)):
        winner = jnp.maximum(former[rank_out], latter[rank_out])
        for rank_in in range(rank_out):
            winner = jnp.maximum(winner, jnp.minimum(former[rank_in], latter[rank_out - rank_in - 1]))
        result.append(winner)
    return tuple(result)

def reference(spectrum):
    table = phase_table(NG)
    cell_count = float(NG * NG * NG)

    def advance(carry, coeffs):
        leaders, running = carry
        score = jnp.dot(coeffs.reshape(NG * NG, 2 * NG), table, precision=lax.Precision.HIGHEST, preferred_element_type=jnp.float32).reshape(NG, NG, NG)
        average = jnp.sum(score) / cell_count
        centred = score - average
        spread = jnp.sum(centred * centred) / cell_count
        normed = centred / jnp.sqrt(spread + SPREAD_FLOOR)
        filler = jnp.full((NG, NG, NG), FLOOR, jnp.float32)
        single = (normed,) + tuple((filler for rank_in in range(TOP - 1)))
        return ((merge_top(leaders, single), running + normed), None)
    start = tuple((jnp.full((NG, NG, NG), FLOOR, jnp.float32) for rank_in in range(TOP)))
    (leaders, running), unused = lax.scan(advance, (start, jnp.zeros((NG, NG, NG), jnp.float32)), spectrum)
    return (jnp.stack(leaders, axis=0), running / math.sqrt(TEMPLATES))
```

```python
import functools
import math

import jax
import jax.numpy as jnp
import numpy as np
from jax import lax
from jax.experimental import pallas as pl
from jax.experimental.pallas import tpu as pltpu
from jax.sharding import Mesh
from jax.sharding import PartitionSpec as P

TOP = 4
SPREAD_FLOOR = 0.25
ROWS = 8
LANES = 128
XY = ("tmpl_0", "tmpl_1")
CORE = "tmpl_2"


def split_table(points):
    order = np.arange(points)
    angle = (order[:, None] * order[None, :] % points) * (2.0 * math.pi / points)
    table = np.concatenate([np.cos(angle), -np.sin(angle)], axis=0)
    mirror = (points - order) % points
    table[:points] = 0.5 * (table[:points] + table[:points][mirror])
    table[points:] = 0.5 * (table[points:] - table[points:][mirror])
    high = table.astype(jnp.bfloat16)
    low = (table - high.astype(np.float64)).astype(jnp.bfloat16)
    pair = [np.kron(np.eye(2), part.astype(np.float64)) for part in (high, low)]
    return np.concatenate(pair, axis=1).astype(jnp.bfloat16)


def to_row(column):
    count = column.shape[0]
    sub = lax.broadcasted_iota(jnp.int32, (count, LANES), 0)
    lane = lax.broadcasted_iota(jnp.int32, (count, LANES), 1)
    return jnp.sum(jnp.where(sub == lane, column, 0.0), axis=0, keepdims=True)


def to_column(row, count):
    sub = lax.broadcasted_iota(jnp.int32, (count, LANES), 0)
    lane = lax.broadcasted_iota(jnp.int32, (count, LANES), 1)
    kept = jnp.sum(jnp.where(sub == lane, row, 0.0), axis=1, keepdims=True)
    return jnp.broadcast_to(kept, (count, LANES))


def score_kernel(x_hbm, w_ref, mine_ref, send_ref, stat_ref, x_vmem, plain, square, sems):
    tmpls, slab, beta, doubled = x_vmem.shape
    pairs = beta // 4
    core = lax.axis_index(CORE)

    def fetch(t):
        return pltpu.make_async_copy(x_hbm.at[t], x_vmem.at[t], sems.at[t])

    for t in range(tmpls):
        fetch(t).start()

    def advance(t, carry):
        fetch(t).wait()
        plain_t = square_t = None
        for parity, out in ((core, mine_ref), (1 - core, send_ref)):
            sides = [
                x_vmem[t, :, pl.ds(2 * parity + h, pairs, stride=4), :].reshape(slab * pairs, doubled)
                for h in range(2)
            ]
            x = jnp.concatenate(sides, axis=1)
            high = x.astype(jnp.bfloat16)
            rest = x - high.astype(jnp.float32)
            mid = rest.astype(jnp.bfloat16)
            low = (rest - mid.astype(jnp.float32)).astype(jnp.bfloat16)
            w = w_ref[...]
            dot = functools.partial(jnp.dot, preferred_element_type=jnp.float32)
            both = dot(low, w) + dot(mid, w) + dot(high, w)
            s = both[:, :LANES] + both[:, LANES:]
            out[t] = s.reshape(slab, pairs, LANES)
            p = jnp.sum(s.reshape(-1, ROWS, LANES), axis=0)
            q = jnp.sum((s * s).reshape(-1, ROWS, LANES), axis=0)
            plain_t = p if plain_t is None else plain_t + p
            square_t = q if square_t is None else square_t + q
        plain[t] = plain_t
        square[t] = square_t
        return carry

    lax.fori_loop(0, tmpls, advance, 0)
    rows = []
    for part in (plain, square):
        whole = jnp.sum(part[...], axis=1)
        rows.append(to_row(jnp.sum(whole, axis=1, keepdims=True)))
    sub = lax.broadcasted_iota(jnp.int32, (ROWS, LANES), 0)
    tile = jnp.where(sub == 0, rows[0], jnp.where(sub == 1, rows[1], 0.0))
    stat_ref[...] = jnp.broadcast_to(tile[None], stat_ref.shape)


def order(a, b):
    return jnp.maximum(a, b), jnp.minimum(a, b)


def sort4(a, b, c, d):
    a, b = order(a, b)
    c, d = order(c, d)
    a, c = order(a, c)
    b, d = order(b, d)
    b, c = order(b, c)
    return a, b, c, d


def merge4(u, v):
    a, b, c, d = (jnp.maximum(u[i], v[3 - i]) for i in range(4))
    a, c = order(a, c)
    b, d = order(b, d)
    a, b = order(a, b)
    c, d = order(c, d)
    return a, b, c, d


def top_kernel(count, mine_ref, other_ref, stat_ref, out_ref, gain_ref, shift_ref):
    tmpls, slab, pairs, _ = mine_ref.shape
    peers = stat_ref.shape[0] // 2
    for half in range(2):
        total = jnp.sum(stat_ref[half * peers : (half + 1) * peers], axis=0)
        average = total[0:1] / count
        spread = total[1:2] / count - average * average
        gain = 1.0 / jnp.sqrt(spread + SPREAD_FLOOR)
        gain_ref[pl.ds(half * tmpls, tmpls)] = to_column(gain, tmpls)
        shift_ref[pl.ds(half * tmpls, tmpls)] = to_column(average, tmpls)
    core = lax.axis_index(CORE)
    firsts = (core * tmpls, (1 - core) * tmpls)

    def tile(a, carry):
        for q in range(pairs // ROWS):
            best = total = None
            for first, ref in zip(firsts, (mine_ref, other_ref)):
                for group in range(tmpls // 4):
                    four = []
                    for t in range(4 * group, 4 * group + 4):
                        s = ref[t, a, pl.ds(q * ROWS, ROWS)]
                        g = gain_ref[pl.ds(first + t, ROWS, stride=0)]
                        m = shift_ref[pl.ds(first + t, ROWS, stride=0)]
                        four.append((s - m) * g)
                    part = (four[0] + four[1]) + (four[2] + four[3])
                    total = part if total is None else total + part
                    four = sort4(*four)
                    best = four if best is None else merge4(best, four)
            for r, value in enumerate((*best, total)):
                start = (q * ROWS * (TOP + 1) + r) * slab + a
                out_ref[pl.ds(start, ROWS, stride=(TOP + 1) * slab)] = value
        return carry

    lax.fori_loop(0, slab, tile, 0)


def final_kernel(norm, in_ref, best_ref, sum_ref):
    peers = in_ref.shape[0]
    points = best_ref.shape[-1]
    fours = [tuple(in_ref[p, r] for r in range(TOP)) for p in range(peers)]
    total = in_ref[0, TOP]
    for p in range(1, peers):
        total = total + in_ref[p, TOP]
    while len(fours) > 1:
        fours = [merge4(u, v) for u, v in zip(fours[::2], fours[1::2])]
    total = total / norm
    for h in range(2):
        lanes = slice(h * points, (h + 1) * points)
        for r in range(TOP):
            best_ref[r, :, h, :] = fours[0][r][:, lanes]
        sum_ref[:, h, :] = total[:, lanes]


def body(spectrum):
    tmpls, slab, beta, doubled = spectrum.shape
    points = doubled // 2
    pairs = beta // 4
    chips = lax.axis_size(XY)
    peers = 2 * lax.axis_size("grid")
    vmem = pl.BlockSpec(memory_space=pltpu.VMEM)
    part = jax.ShapeDtypeStruct((tmpls, slab, pairs, LANES), jnp.float32)
    mine, send, stat = pl.pallas_call(
        score_kernel,
        out_shape=(part, part, jax.ShapeDtypeStruct((peers, ROWS, LANES), jnp.float32)),
        in_specs=[pl.BlockSpec(memory_space=pl.ANY), vmem],
        out_specs=(vmem, vmem, vmem),
        scratch_shapes=[
            pltpu.VMEM(spectrum.shape, jnp.float32),
            pltpu.VMEM((tmpls, ROWS, LANES), jnp.float32),
            pltpu.VMEM((tmpls, ROWS, LANES), jnp.float32),
            pltpu.SemaphoreType.DMA((tmpls,)),
        ],
        compiler_params=pltpu.CompilerParams(vmem_limit_bytes=40 * 2**20),
        name="scores",
    )(spectrum, jnp.asarray(split_table(points)))
    stats = lax.all_to_all(stat, (CORE, "grid"), split_axis=0, concat_axis=0, tiled=True)
    other = lax.ppermute(send, CORE, [(0, 1), (1, 0)])
    packed = pl.pallas_call(
        functools.partial(top_kernel, float(points**3)),
        out_shape=jax.ShapeDtypeStruct((chips * (TOP + 1) * slab, LANES), jnp.float32),
        in_specs=[vmem, vmem, vmem],
        out_specs=vmem,
        scratch_shapes=[
            pltpu.VMEM((2 * tmpls, LANES), jnp.float32),
            pltpu.VMEM((2 * tmpls, LANES), jnp.float32),
        ],
        compiler_params=pltpu.CompilerParams(vmem_limit_bytes=20 * 2**20),
        name="tops",
    )(mine, other, stats)
    packed = packed.reshape(chips, TOP + 1, slab, LANES)
    received = lax.all_to_all(packed, XY, split_axis=0, concat_axis=0, tiled=True)
    return pl.pallas_call(
        functools.partial(final_kernel, math.sqrt(2 * chips * tmpls)),
        out_shape=(
            jax.ShapeDtypeStruct((TOP, slab, 2, points), jnp.float32),
            jax.ShapeDtypeStruct((slab, 2, points), jnp.float32),
        ),
        in_specs=[vmem],
        out_specs=(vmem, vmem),
        name="finish",
    )(received)


def solution(mesh):
    finer = Mesh(
        mesh.devices.reshape(4, 4, 2, mesh.shape["grid"]), (*XY, CORE, "grid")
    )
    tmpl = (*XY, CORE)
    return jax.shard_map(
        body,
        mesh=finer,
        in_specs=(P(tmpl, "grid", None, None),),
        out_specs=(P(None, "grid", tmpl, None), P("grid", tmpl, None)),
        check_vma=False,
    )
```

```python
import functools
import math

import jax
import jax.numpy as jnp
import numpy as np
from jax import lax
from jax.experimental import pallas as pl
from jax.experimental.pallas import tpu as pltpu
from jax.sharding import Mesh
from jax.sharding import PartitionSpec as P

TOP = 4
SPREAD_FLOOR = 0.25
ROWS = 8
LANES = 128
GROUP = 4
XY = ("tmpl_0", "tmpl_1")
CORE = "tmpl_2"


def split_table(points):
    order = np.arange(points)
    angle = (order[:, None] * order[None, :] % points) * (2.0 * math.pi / points)
    table = np.concatenate([np.cos(angle), -np.sin(angle)], axis=0)
    mirror = (points - order) % points
    table[:points] = 0.5 * (table[:points] + table[:points][mirror])
    table[points:] = 0.5 * (table[points:] - table[points:][mirror])
    high = table.astype(jnp.bfloat16)
    low = (table - high.astype(np.float64)).astype(jnp.bfloat16)
    pair = [np.kron(np.eye(2), part.astype(np.float64)) for part in (high, low)]
    return np.concatenate(pair, axis=1).astype(jnp.bfloat16)


def to_row(column):
    count = column.shape[0]
    sub = lax.broadcasted_iota(jnp.int32, (count, LANES), 0)
    lane = lax.broadcasted_iota(jnp.int32, (count, LANES), 1)
    return jnp.sum(jnp.where(sub == lane, column, 0.0), axis=0, keepdims=True)


def to_column(row, count):
    sub = lax.broadcasted_iota(jnp.int32, (count, LANES), 0)
    lane = lax.broadcasted_iota(jnp.int32, (count, LANES), 1)
    kept = jnp.sum(jnp.where(sub == lane, row, 0.0), axis=1, keepdims=True)
    return jnp.broadcast_to(kept, (count, LANES))


def score_kernel(
    x_hbm, w_hbm, mine_ref, send_ref, stat_ref, x_vmem, w_vmem, plain, square, sems, w_sem
):
    tmpls, slab, beta, doubled = x_vmem.shape
    pairs = beta // 4
    rows = slab * pairs
    core = lax.axis_index(CORE)
    parities = (core, 1 - core)
    outs = (mine_ref, send_ref)

    def fetch(g):
        block = pl.ds(g * GROUP, GROUP)
        return pltpu.make_async_copy(x_hbm.at[block], x_vmem.at[block], sems.at[g])

    table = pltpu.make_async_copy(w_hbm, w_vmem, w_sem)
    table.start()
    for g in range(tmpls // GROUP):
        fetch(g).start()
    table.wait()

    def parts(t, parity):
        sides = [
            x_vmem[t, :, pl.ds(2 * parity + h, pairs, stride=4), :].reshape(rows, doubled)
            for h in range(2)
        ]
        x = jnp.concatenate(sides, axis=1)
        high = x.astype(jnp.bfloat16)
        rest = x - high.astype(jnp.float32)
        mid = rest.astype(jnp.bfloat16)
        low = (rest - mid.astype(jnp.float32)).astype(jnp.bfloat16)
        return low, mid, high

    def run(*accs):
        first, accs = accs[:2], accs[2:]
        for m in range(2):
            pltpu.matmul_push_rhs(w_vmem[...], staging_register=0, mxu_index=m)
            zeros = jnp.zeros((16, 2 * doubled), jnp.bfloat16)
            pltpu.matmul_acc_lhs(first[m], zeros, load_staged_rhs=0)
            pltpu.matmul_pop(first[m])

        def take(t, u):
            plain_t = square_t = None
            for m in range(2):
                both = pltpu.matmul_pop(accs[2 * u + m])
                s = both[:, :LANES] + both[:, LANES:]
                outs[m][t] = s.reshape(slab, pairs, LANES)
                p = jnp.sum(s.reshape(-1, ROWS, LANES), axis=0)
                q = jnp.sum((s * s).reshape(-1, ROWS, LANES), axis=0)
                plain_t = p if plain_t is None else plain_t + p
                square_t = q if square_t is None else square_t + q
            plain[t] = plain_t
            square[t] = square_t

        def advance(g, carry):
            fetch(g).wait()
            for u in range(GROUP):
                for m in range(2):
                    for part in parts(g * GROUP + u, parities[m]):
                        pltpu.matmul_acc_lhs(accs[2 * (u % 4) + m], part)
                if u:
                    take(g * GROUP + u - 1, (u - 1) % 4)
            take(g * GROUP + GROUP - 1, (GROUP - 1) % 4)
            return carry

        lax.fori_loop(0, tmpls // GROUP, advance, 0)

    pl.run_scoped(
        run,
        *(pltpu.ACC(m)((16, 256), jnp.float32) for m in range(2)),
        *(pltpu.ACC(m)((rows, 256), jnp.float32) for _ in range(4) for m in range(2)),
    )
    totals = []
    for part in (plain, square):
        whole = jnp.sum(part[...], axis=1)
        totals.append(to_row(jnp.sum(whole, axis=1, keepdims=True)))
    sub = lax.broadcasted_iota(jnp.int32, (ROWS, LANES), 0)
    tile = jnp.where(sub == 0, totals[0], jnp.where(sub == 1, totals[1], 0.0))
    stat_ref[...] = jnp.broadcast_to(tile[None], stat_ref.shape)


def order(a, b):
    return jnp.maximum(a, b), jnp.minimum(a, b)


def sort4(a, b, c, d):
    a, b = order(a, b)
    c, d = order(c, d)
    a, c = order(a, c)
    b, d = order(b, d)
    b, c = order(b, c)
    return a, b, c, d


def merge4(u, v):
    a, b, c, d = (jnp.maximum(u[i], v[3 - i]) for i in range(4))
    a, c = order(a, c)
    b, d = order(b, d)
    a, b = order(a, b)
    c, d = order(c, d)
    return a, b, c, d


def top_kernel(count, mine_ref, other_ref, stat_ref, out_ref, gain_ref, shift_ref):
    tmpls, slab, pairs, _ = mine_ref.shape
    peers = stat_ref.shape[0] // 2
    for half in range(2):
        total = jnp.sum(stat_ref[half * peers : (half + 1) * peers], axis=0)
        average = total[0:1] / count
        spread = total[1:2] / count - average * average
        gain = 1.0 / jnp.sqrt(spread + SPREAD_FLOOR)
        gain_ref[pl.ds(half * tmpls, tmpls)] = to_column(gain, tmpls)
        shift_ref[pl.ds(half * tmpls, tmpls)] = to_column(average, tmpls)
    core = lax.axis_index(CORE)
    firsts = (core * tmpls, (1 - core) * tmpls)

    def tile(a, carry):
        for q in range(pairs // ROWS):
            best = total = None
            for first, ref in zip(firsts, (mine_ref, other_ref)):
                for group in range(tmpls // 4):
                    four = []
                    for t in range(4 * group, 4 * group + 4):
                        s = ref[t, a, pl.ds(q * ROWS, ROWS)]
                        g = gain_ref[pl.ds(first + t, ROWS, stride=0)]
                        m = shift_ref[pl.ds(first + t, ROWS, stride=0)]
                        four.append((s - m) * g)
                    part = (four[0] + four[1]) + (four[2] + four[3])
                    total = part if total is None else total + part
                    four = sort4(*four)
                    best = four if best is None else merge4(best, four)
            for r, value in enumerate((*best, total)):
                start = (q * ROWS * (TOP + 1) + r) * slab + a
                out_ref[pl.ds(start, ROWS, stride=(TOP + 1) * slab)] = value
        return carry

    lax.fori_loop(0, slab, tile, 0)


def final_kernel(norm, in_ref, best_ref, sum_ref):
    peers = in_ref.shape[0]
    points = best_ref.shape[-1]
    fours = [tuple(in_ref[p, r] for r in range(TOP)) for p in range(peers)]
    total = in_ref[0, TOP]
    for p in range(1, peers):
        total = total + in_ref[p, TOP]
    while len(fours) > 1:
        fours = [merge4(u, v) for u, v in zip(fours[::2], fours[1::2])]
    total = total / norm
    for h in range(2):
        lanes = slice(h * points, (h + 1) * points)
        for r in range(TOP):
            best_ref[r, :, h, :] = fours[0][r][:, lanes]
        sum_ref[:, h, :] = total[:, lanes]


def body(spectrum):
    tmpls, slab, beta, doubled = spectrum.shape
    points = doubled // 2
    pairs = beta // 4
    chips = lax.axis_size(XY)
    peers = 2 * lax.axis_size("grid")
    vmem = pl.BlockSpec(memory_space=pltpu.VMEM)
    part = jax.ShapeDtypeStruct((tmpls, slab, pairs, LANES), jnp.float32)
    mine, send, stat = pl.pallas_call(
        score_kernel,
        out_shape=(part, part, jax.ShapeDtypeStruct((peers, ROWS, LANES), jnp.float32)),
        in_specs=[pl.BlockSpec(memory_space=pltpu.HBM)] * 2,
        out_specs=(vmem, vmem, vmem),
        scratch_shapes=[
            pltpu.VMEM(spectrum.shape, jnp.float32),
            pltpu.VMEM((2 * doubled, 2 * doubled), jnp.bfloat16),
            pltpu.VMEM((tmpls, ROWS, LANES), jnp.float32),
            pltpu.VMEM((tmpls, ROWS, LANES), jnp.float32),
            pltpu.SemaphoreType.DMA((tmpls // GROUP,)),
            pltpu.SemaphoreType.DMA,
        ],
        compiler_params=pltpu.CompilerParams(vmem_limit_bytes=40 * 2**20),
        name="scores",
    )(*(
        pltpu.with_memory_space_constraint(a, pltpu.HBM)
        for a in (spectrum, jnp.asarray(split_table(points)))
    ))
    stats = lax.all_to_all(stat, (CORE, "grid"), split_axis=0, concat_axis=0, tiled=True)
    other = lax.ppermute(send, CORE, [(0, 1), (1, 0)])
    packed = pl.pallas_call(
        functools.partial(top_kernel, float(points**3)),
        out_shape=jax.ShapeDtypeStruct((chips * (TOP + 1) * slab, LANES), jnp.float32),
        in_specs=[vmem, vmem, vmem],
        out_specs=vmem,
        scratch_shapes=[
            pltpu.VMEM((2 * tmpls, LANES), jnp.float32),
            pltpu.VMEM((2 * tmpls, LANES), jnp.float32),
        ],
        compiler_params=pltpu.CompilerParams(vmem_limit_bytes=20 * 2**20),
        name="tops",
    )(mine, other, stats)
    packed = packed.reshape(chips, TOP + 1, slab, LANES)
    received = lax.all_to_all(packed, XY, split_axis=0, concat_axis=0, tiled=True)
    return pl.pallas_call(
        functools.partial(final_kernel, math.sqrt(2 * chips * tmpls)),
        out_shape=(
            jax.ShapeDtypeStruct((TOP, slab, 2, points), jnp.float32),
            jax.ShapeDtypeStruct((slab, 2, points), jnp.float32),
        ),
        in_specs=[vmem],
        out_specs=(vmem, vmem),
        compiler_params=pltpu.CompilerParams(vmem_limit_bytes=8 * 2**20),
        name="finish",
    )(received)


def solution(mesh):
    finer = Mesh(
        mesh.devices.reshape(4, 4, 2, mesh.shape["grid"]), (*XY, CORE, "grid")
    )
    tmpl = (*XY, CORE)
    return jax.shard_map(
        body,
        mesh=finer,
        in_specs=(P(tmpl, "grid", None, None),),
        out_specs=(P(None, "grid", tmpl, None), P("grid", tmpl, None)),
        check_vma=False,
    )
```

```python
import functools
import math

import jax
import jax.numpy as jnp
import numpy as np
from jax import lax
from jax.experimental import pallas as pl
from jax.experimental.pallas import tpu as pltpu
from jax.sharding import Mesh
from jax.sharding import PartitionSpec as P

TOP = 4
SPREAD_FLOOR = 0.25
ROWS = 8
LANES = 128
CHUNKS = (4,) * 8
AHEAD = {0: 6, 1: 8}
FIRST = 3
LIVE = 4
XY = ("tmpl_0", "tmpl_1")
CORE = "tmpl_2"


def split_table(points):
    order = np.arange(points)
    angle = (order[:, None] * order[None, :] % points) * (2.0 * math.pi / points)
    table = np.concatenate([np.cos(angle), -np.sin(angle)], axis=0)
    mirror = (points - order) % points
    table[:points] = 0.5 * (table[:points] + table[:points][mirror])
    table[points:] = 0.5 * (table[points:] - table[points:][mirror])
    high = table.astype(jnp.bfloat16)
    low = (table - high.astype(np.float64)).astype(jnp.bfloat16)
    pair = [np.kron(np.eye(2), part.astype(np.float64)) for part in (high, low)]
    return np.concatenate(pair, axis=1).astype(jnp.bfloat16)


def to_row(column):
    count = column.shape[0]
    sub = lax.broadcasted_iota(jnp.int32, (count, LANES), 0)
    lane = lax.broadcasted_iota(jnp.int32, (count, LANES), 1)
    return jnp.sum(jnp.where(sub == lane, column, 0.0), axis=0, keepdims=True)


def to_column(row, count):
    sub = lax.broadcasted_iota(jnp.int32, (count, LANES), 0)
    lane = lax.broadcasted_iota(jnp.int32, (count, LANES), 1)
    kept = jnp.sum(jnp.where(sub == lane, row, 0.0), axis=1, keepdims=True)
    return jnp.broadcast_to(kept, (count, LANES))


def score_kernel(
    x_hbm, w_hbm, mine_ref, send_ref, stat_ref, x_vmem, w_vmem, plain, square, sems, w_sem
):
    tmpls, slab, beta, doubled = x_vmem.shape
    pairs = beta // 4
    rows = slab * pairs
    core = lax.axis_index(CORE)
    parities = (core, 1 - core)
    outs = (mine_ref, send_ref)

    edges = [sum(CHUNKS[:c]) for c in range(len(CHUNKS) + 1)]
    started = [0]

    def fetch(c):
        block = pl.ds(edges[c], CHUNKS[c])
        return pltpu.make_async_copy(x_hbm.at[block], x_vmem.at[block], sems.at[c])

    def fetch_up_to(c):
        for ahead in range(started[0], c):
            fetch(ahead).start()
        started[0] = max(started[0], c)

    table = pltpu.make_async_copy(w_hbm, w_vmem, w_sem)
    table.start()
    fetch_up_to(FIRST)
    table.wait()

    def parts(t, parity):
        sides = [
            x_vmem[t, :, pl.ds(2 * parity + h, pairs, stride=4), :].reshape(rows, doubled)
            for h in range(2)
        ]
        x = jnp.concatenate(sides, axis=1)
        high = x.astype(jnp.bfloat16)
        rest = x - high.astype(jnp.float32)
        mid = rest.astype(jnp.bfloat16)
        low = (rest - mid.astype(jnp.float32)).astype(jnp.bfloat16)
        return low, mid, high

    def run(*accs):
        first, accs = accs[:2], accs[2:]
        for m in range(2):
            pltpu.matmul_push_rhs(w_vmem[...], staging_register=0, mxu_index=m)
            zeros = jnp.zeros((16, 2 * doubled), jnp.bfloat16)
            pltpu.matmul_acc_lhs(first[m], zeros, load_staged_rhs=0)
            pltpu.matmul_pop(first[m])

        def take(t, u):
            plain_t = square_t = None
            for m in range(2):
                both = pltpu.matmul_pop(accs[2 * u + m])
                s = both[:, :LANES] + both[:, LANES:]
                outs[m][t] = s.reshape(slab, pairs, LANES)
                p = jnp.sum(s.reshape(-1, ROWS, LANES), axis=0)
                q = jnp.sum((s * s).reshape(-1, ROWS, LANES), axis=0)
                plain_t = p if plain_t is None else plain_t + p
                square_t = q if square_t is None else square_t + q
            plain[t] = plain_t
            square[t] = square_t

        for t in range(tmpls):
            if t in edges:
                c = edges.index(t)
                fetch(c).wait()
                fetch_up_to(AHEAD.get(c, 0))
            for m in range(2):
                for part in parts(t, parities[m]):
                    pltpu.matmul_acc_lhs(accs[2 * (t % LIVE) + m], part)
            if t:
                take(t - 1, (t - 1) % LIVE)
        take(tmpls - 1, (tmpls - 1) % LIVE)

    pl.run_scoped(
        run,
        *(pltpu.ACC(m)((16, 256), jnp.float32) for m in range(2)),
        *(pltpu.ACC(m)((rows, 256), jnp.float32) for _ in range(LIVE) for m in range(2)),
    )
    totals = []
    for part in (plain, square):
        whole = jnp.sum(part[...], axis=1)
        totals.append(to_row(jnp.sum(whole, axis=1, keepdims=True)))
    sub = lax.broadcasted_iota(jnp.int32, (ROWS, LANES), 0)
    tile = jnp.where(sub == 0, totals[0], jnp.where(sub == 1, totals[1], 0.0))
    stat_ref[...] = jnp.broadcast_to(tile[None], stat_ref.shape)


def order(a, b):
    return jnp.maximum(a, b), jnp.minimum(a, b)


def sort4(a, b, c, d):
    a, b = order(a, b)
    c, d = order(c, d)
    a, c = order(a, c)
    b, d = order(b, d)
    b, c = order(b, c)
    return a, b, c, d


def merge4(u, v):
    a, b, c, d = (jnp.maximum(u[i], v[3 - i]) for i in range(4))
    a, c = order(a, c)
    b, d = order(b, d)
    a, b = order(a, b)
    c, d = order(c, d)
    return a, b, c, d


def top_kernel(count, mine_ref, other_ref, stat_ref, out_ref, gain_ref, shift_ref):
    tmpls, slab, pairs, _ = mine_ref.shape
    peers = stat_ref.shape[0] // 2
    for half in range(2):
        total = jnp.sum(stat_ref[half * peers : (half + 1) * peers], axis=0)
        average = total[0:1] / count
        spread = total[1:2] / count - average * average
        gain = 1.0 / jnp.sqrt(spread + SPREAD_FLOOR)
        gain_ref[pl.ds(half * tmpls, tmpls)] = to_column(gain, tmpls)
        shift_ref[pl.ds(half * tmpls, tmpls)] = to_column(average, tmpls)
    core = lax.axis_index(CORE)
    firsts = (core * tmpls, (1 - core) * tmpls)

    def tile(a, carry):
        for q in range(pairs // ROWS):
            best = total = None
            for first, ref in zip(firsts, (mine_ref, other_ref)):
                for group in range(tmpls // 4):
                    four = []
                    for t in range(4 * group, 4 * group + 4):
                        s = ref[t, a, pl.ds(q * ROWS, ROWS)]
                        g = gain_ref[pl.ds(first + t, ROWS, stride=0)]
                        m = shift_ref[pl.ds(first + t, ROWS, stride=0)]
                        four.append((s - m) * g)
                    part = (four[0] + four[1]) + (four[2] + four[3])
                    total = part if total is None else total + part
                    four = sort4(*four)
                    best = four if best is None else merge4(best, four)
            for r, value in enumerate((*best, total)):
                start = (q * ROWS * (TOP + 1) + r) * slab + a
                out_ref[pl.ds(start, ROWS, stride=(TOP + 1) * slab)] = value
        return carry

    lax.fori_loop(0, slab, tile, 0)


def final_kernel(norm, in_ref, best_ref, sum_ref):
    peers = in_ref.shape[0]
    points = best_ref.shape[-1]
    fours = [tuple(in_ref[p, r] for r in range(TOP)) for p in range(peers)]
    total = in_ref[0, TOP]
    for p in range(1, peers):
        total = total + in_ref[p, TOP]
    while len(fours) > 1:
        fours = [merge4(u, v) for u, v in zip(fours[::2], fours[1::2])]
    total = total / norm
    for h in range(2):
        lanes = slice(h * points, (h + 1) * points)
        for r in range(TOP):
            best_ref[r, :, h, :] = fours[0][r][:, lanes]
        sum_ref[:, h, :] = total[:, lanes]


def body(spectrum):
    tmpls, slab, beta, doubled = spectrum.shape
    points = doubled // 2
    pairs = beta // 4
    chips = lax.axis_size(XY)
    peers = 2 * lax.axis_size("grid")
    vmem = pl.BlockSpec(memory_space=pltpu.VMEM)
    part = jax.ShapeDtypeStruct((tmpls, slab, pairs, LANES), jnp.float32)
    mine, send, stat = pl.pallas_call(
        score_kernel,
        out_shape=(part, part, jax.ShapeDtypeStruct((peers, ROWS, LANES), jnp.float32)),
        in_specs=[pl.BlockSpec(memory_space=pltpu.HBM)] * 2,
        out_specs=(vmem, vmem, vmem),
        scratch_shapes=[
            pltpu.VMEM(spectrum.shape, jnp.float32),
            pltpu.VMEM((2 * doubled, 2 * doubled), jnp.bfloat16),
            pltpu.VMEM((tmpls, ROWS, LANES), jnp.float32),
            pltpu.VMEM((tmpls, ROWS, LANES), jnp.float32),
            pltpu.SemaphoreType.DMA((len(CHUNKS),)),
            pltpu.SemaphoreType.DMA,
        ],
        compiler_params=pltpu.CompilerParams(vmem_limit_bytes=40 * 2**20),
        name="scores",
    )(*(
        pltpu.with_memory_space_constraint(a, pltpu.HBM)
        for a in (spectrum, jnp.asarray(split_table(points)))
    ))
    stats = lax.all_to_all(stat, (CORE, "grid"), split_axis=0, concat_axis=0, tiled=True)
    other = lax.ppermute(send, CORE, [(0, 1), (1, 0)])
    packed = pl.pallas_call(
        functools.partial(top_kernel, float(points**3)),
        out_shape=jax.ShapeDtypeStruct((chips * (TOP + 1) * slab, LANES), jnp.float32),
        in_specs=[vmem, vmem, vmem],
        out_specs=vmem,
        scratch_shapes=[
            pltpu.VMEM((2 * tmpls, LANES), jnp.float32),
            pltpu.VMEM((2 * tmpls, LANES), jnp.float32),
        ],
        compiler_params=pltpu.CompilerParams(vmem_limit_bytes=20 * 2**20),
        name="tops",
    )(mine, other, stats)
    packed = packed.reshape(chips, TOP + 1, slab, LANES)
    received = lax.all_to_all(packed, XY, split_axis=0, concat_axis=0, tiled=True)
    return pl.pallas_call(
        functools.partial(final_kernel, math.sqrt(2 * chips * tmpls)),
        out_shape=(
            jax.ShapeDtypeStruct((TOP, slab, 2, points), jnp.float32),
            jax.ShapeDtypeStruct((slab, 2, points), jnp.float32),
        ),
        in_specs=[vmem],
        out_specs=(vmem, vmem),
        compiler_params=pltpu.CompilerParams(vmem_limit_bytes=8 * 2**20),
        name="finish",
    )(received)


def solution(mesh):
    finer = Mesh(
        mesh.devices.reshape(4, 4, 2, mesh.shape["grid"]), (*XY, CORE, "grid")
    )
    tmpl = (*XY, CORE)
    return jax.shard_map(
        body,
        mesh=finer,
        in_specs=(P(tmpl, "grid", None, None),),
        out_specs=(P(None, "grid", tmpl, None), P("grid", tmpl, None)),
        check_vma=False,
    )
```

```python
import functools
import math

import jax
import jax.numpy as jnp
import numpy as np
from jax import lax
from jax.experimental import pallas as pl
from jax.experimental.pallas import tpu as pltpu
from jax.sharding import Mesh
from jax.sharding import PartitionSpec as P

TOP = 4
SPREAD_FLOOR = 0.25
ROWS = 8
LANES = 128
CHUNKS = (4,) * 8
AHEAD = {0: 6, 1: 8}
FIRST = 3
LIVE = 4
STAT_ORDER = [(c, z) for c in (1, 0) for z in (4, 5, 6, 7, 0, 1, 2, 3)]
CHIP_ORDER = (10, 15, 14, 11, 9, 6, 13, 7, 12, 8, 5, 3, 2, 4, 1, 0)
XY = ("tmpl_0", "tmpl_1")
CORE = "tmpl_2"


def split_table(points):
    order = np.arange(points)
    angle = (order[:, None] * order[None, :] % points) * (2.0 * math.pi / points)
    table = np.concatenate([np.cos(angle), -np.sin(angle)], axis=0)
    mirror = (points - order) % points
    table[:points] = 0.5 * (table[:points] + table[:points][mirror])
    table[points:] = 0.5 * (table[points:] - table[points:][mirror])
    high = table.astype(jnp.bfloat16)
    low = (table - high.astype(np.float64)).astype(jnp.bfloat16)
    pair = [np.kron(np.eye(2), part.astype(np.float64)) for part in (high, low)]
    return np.concatenate(pair, axis=1).astype(jnp.bfloat16)


def to_row(column):
    count = column.shape[0]
    sub = lax.broadcasted_iota(jnp.int32, (count, LANES), 0)
    lane = lax.broadcasted_iota(jnp.int32, (count, LANES), 1)
    return jnp.sum(jnp.where(sub == lane, column, 0.0), axis=0, keepdims=True)


def to_column(row, count):
    sub = lax.broadcasted_iota(jnp.int32, (count, LANES), 0)
    lane = lax.broadcasted_iota(jnp.int32, (count, LANES), 1)
    kept = jnp.sum(jnp.where(sub == lane, row, 0.0), axis=1, keepdims=True)
    return jnp.broadcast_to(kept, (count, LANES))


def score_kernel(
    x_hbm, w_hbm, mine_ref, send_ref, stat_ref, x_vmem, w_vmem, plain, square, sems, w_sem
):
    tmpls, slab, beta, doubled = x_vmem.shape
    pairs = beta // 4
    rows = slab * pairs
    core = lax.axis_index(CORE)
    parities = (core, 1 - core)
    outs = (mine_ref, send_ref)

    edges = [sum(CHUNKS[:c]) for c in range(len(CHUNKS) + 1)]
    started = [0]

    def fetch(c):
        block = pl.ds(edges[c], CHUNKS[c])
        return pltpu.make_async_copy(x_hbm.at[block], x_vmem.at[block], sems.at[c])

    def fetch_up_to(c):
        for ahead in range(started[0], c):
            fetch(ahead).start()
        started[0] = max(started[0], c)

    table = pltpu.make_async_copy(w_hbm, w_vmem, w_sem)
    table.start()
    fetch_up_to(FIRST)
    table.wait()

    def parts(t, parity):
        sides = [
            x_vmem[t, :, pl.ds(2 * parity + h, pairs, stride=4), :].reshape(rows, doubled)
            for h in range(2)
        ]
        x = jnp.concatenate(sides, axis=1)
        high = x.astype(jnp.bfloat16)
        rest = x - high.astype(jnp.float32)
        mid = rest.astype(jnp.bfloat16)
        low = (rest - mid.astype(jnp.float32)).astype(jnp.bfloat16)
        return low, mid, high

    def run(*accs):
        first, accs = accs[:2], accs[2:]
        for m in range(2):
            pltpu.matmul_push_rhs(w_vmem[...], staging_register=0, mxu_index=m)
            zeros = jnp.zeros((16, 2 * doubled), jnp.bfloat16)
            pltpu.matmul_acc_lhs(first[m], zeros, load_staged_rhs=0)
            pltpu.matmul_pop(first[m])

        def take(t, u):
            plain_t = square_t = None
            for m in range(2):
                both = pltpu.matmul_pop(accs[2 * u + m])
                s = both[:, :LANES] + both[:, LANES:]
                outs[m][t] = s.reshape(slab, pairs, LANES)
                p = jnp.sum(s.reshape(-1, ROWS, LANES), axis=0)
                q = jnp.sum((s * s).reshape(-1, ROWS, LANES), axis=0)
                plain_t = p if plain_t is None else plain_t + p
                square_t = q if square_t is None else square_t + q
            plain[t] = plain_t
            square[t] = square_t

        for t in range(tmpls):
            if t in edges:
                c = edges.index(t)
                fetch(c).wait()
                fetch_up_to(AHEAD.get(c, 0))
            for m in range(2):
                for part in parts(t, parities[m]):
                    pltpu.matmul_acc_lhs(accs[2 * (t % LIVE) + m], part)
            if t:
                take(t - 1, (t - 1) % LIVE)
        take(tmpls - 1, (tmpls - 1) % LIVE)

    pl.run_scoped(
        run,
        *(pltpu.ACC(m)((16, 256), jnp.float32) for m in range(2)),
        *(pltpu.ACC(m)((rows, 256), jnp.float32) for _ in range(LIVE) for m in range(2)),
    )
    totals = []
    for part in (plain, square):
        whole = jnp.sum(part[...], axis=1)
        totals.append(to_row(jnp.sum(whole, axis=1, keepdims=True)))
    sub = lax.broadcasted_iota(jnp.int32, (ROWS, LANES), 0)
    tile = jnp.where(sub == 0, totals[0], jnp.where(sub == 1, totals[1], 0.0))
    stat_ref[...] = jnp.broadcast_to(tile[None], stat_ref.shape)


def order(a, b):
    return jnp.maximum(a, b), jnp.minimum(a, b)


def sort4(a, b, c, d):
    a, b = order(a, b)
    c, d = order(c, d)
    a, c = order(a, c)
    b, d = order(b, d)
    b, c = order(b, c)
    return a, b, c, d


def merge4(u, v):
    a, b, c, d = (jnp.maximum(u[i], v[3 - i]) for i in range(4))
    a, c = order(a, c)
    b, d = order(b, d)
    a, b = order(a, b)
    c, d = order(c, d)
    return a, b, c, d


def top_kernel(count, mine_ref, other_ref, stat_ref, out_ref, gain_ref, shift_ref, staged):
    tmpls, slab, pairs, _ = mine_ref.shape
    for half in range(2):
        total = sum(stat_ref[p] for p, (c, _) in enumerate(STAT_ORDER) if c == half)
        average = total[0:1] / count
        spread = total[1:2] / count - average * average
        gain = 1.0 / jnp.sqrt(spread + SPREAD_FLOOR)
        gain_ref[pl.ds(half * tmpls, tmpls)] = to_column(gain, tmpls)
        shift_ref[pl.ds(half * tmpls, tmpls)] = to_column(average, tmpls)
    core = lax.axis_index(CORE)
    firsts = (core * tmpls, (1 - core) * tmpls)

    def tile(a, carry):
        for q in range(pairs // ROWS):
            best = total = None
            for first, ref in zip(firsts, (mine_ref, other_ref)):
                for group in range(tmpls // 4):
                    four = []
                    for t in range(4 * group, 4 * group + 4):
                        s = ref[t, a, pl.ds(q * ROWS, ROWS)]
                        g = gain_ref[pl.ds(first + t, ROWS, stride=0)]
                        m = shift_ref[pl.ds(first + t, ROWS, stride=0)]
                        four.append((s - m) * g)
                    part = (four[0] + four[1]) + (four[2] + four[3])
                    total = part if total is None else total + part
                    four = sort4(*four)
                    best = four if best is None else merge4(best, four)
            for r, value in enumerate((*best, total)):
                start = (q * ROWS * (TOP + 1) + r) * slab + a
                staged[pl.ds(start, ROWS, stride=(TOP + 1) * slab)] = value
        return carry

    lax.fori_loop(0, slab, tile, 0)
    size = (TOP + 1) * slab
    for place, chip in enumerate(CHIP_ORDER):
        out_ref[place * size : (place + 1) * size] = staged[chip * size : (chip + 1) * size]


def final_kernel(norm, in_ref, best_ref, sum_ref):
    peers = in_ref.shape[0]
    points = best_ref.shape[-1]
    fours = [tuple(in_ref[p, r] for r in range(TOP)) for p in range(peers)]
    total = in_ref[0, TOP]
    for p in range(1, peers):
        total = total + in_ref[p, TOP]
    while len(fours) > 1:
        fours = [merge4(u, v) for u, v in zip(fours[::2], fours[1::2])]
    total = total / norm
    for h in range(2):
        lanes = slice(h * points, (h + 1) * points)
        for r in range(TOP):
            best_ref[r, :, h, :] = fours[0][r][:, lanes]
        sum_ref[:, h, :] = total[:, lanes]


def body(spectrum):
    tmpls, slab, beta, doubled = spectrum.shape
    points = doubled // 2
    pairs = beta // 4
    chips = lax.axis_size(XY)
    peers = 2 * lax.axis_size("grid")
    vmem = pl.BlockSpec(memory_space=pltpu.VMEM)
    part = jax.ShapeDtypeStruct((tmpls, slab, pairs, LANES), jnp.float32)
    mine, send, stat = pl.pallas_call(
        score_kernel,
        out_shape=(part, part, jax.ShapeDtypeStruct((peers, ROWS, LANES), jnp.float32)),
        in_specs=[pl.BlockSpec(memory_space=pltpu.HBM)] * 2,
        out_specs=(vmem, vmem, vmem),
        scratch_shapes=[
            pltpu.VMEM(spectrum.shape, jnp.float32),
            pltpu.VMEM((2 * doubled, 2 * doubled), jnp.bfloat16),
            pltpu.VMEM((tmpls, ROWS, LANES), jnp.float32),
            pltpu.VMEM((tmpls, ROWS, LANES), jnp.float32),
            pltpu.SemaphoreType.DMA((len(CHUNKS),)),
            pltpu.SemaphoreType.DMA,
        ],
        compiler_params=pltpu.CompilerParams(vmem_limit_bytes=40 * 2**20),
        name="scores",
    )(*(
        pltpu.with_memory_space_constraint(a, pltpu.HBM)
        for a in (spectrum, jnp.asarray(split_table(points)))
    ))
    meeting = [[c * lax.axis_size("grid") + z for c, z in STAT_ORDER]]
    stats = lax.all_to_all(
        stat, (CORE, "grid"), split_axis=0, concat_axis=0, axis_index_groups=meeting, tiled=True
    )
    other = lax.ppermute(send, CORE, [(0, 1), (1, 0)])
    packed = pl.pallas_call(
        functools.partial(top_kernel, float(points**3)),
        out_shape=jax.ShapeDtypeStruct((chips * (TOP + 1) * slab, LANES), jnp.float32),
        in_specs=[vmem, vmem, vmem],
        out_specs=vmem,
        scratch_shapes=[
            pltpu.VMEM((2 * tmpls, LANES), jnp.float32),
            pltpu.VMEM((2 * tmpls, LANES), jnp.float32),
            pltpu.VMEM((chips * (TOP + 1) * slab, LANES), jnp.float32),
        ],
        compiler_params=pltpu.CompilerParams(vmem_limit_bytes=20 * 2**20),
        name="tops",
    )(mine, other, stats)
    packed = packed.reshape(chips, TOP + 1, slab, LANES)
    received = lax.all_to_all(
        packed, XY, split_axis=0, concat_axis=0, axis_index_groups=[list(CHIP_ORDER)], tiled=True
    )
    return pl.pallas_call(
        functools.partial(final_kernel, math.sqrt(2 * chips * tmpls)),
        out_shape=(
            jax.ShapeDtypeStruct((TOP, slab, 2, points), jnp.float32),
            jax.ShapeDtypeStruct((slab, 2, points), jnp.float32),
        ),
        in_specs=[vmem],
        out_specs=(vmem, vmem),
        compiler_params=pltpu.CompilerParams(vmem_limit_bytes=8 * 2**20),
        name="finish",
    )(received)


def solution(mesh):
    finer = Mesh(
        mesh.devices.reshape(4, 4, 2, mesh.shape["grid"]), (*XY, CORE, "grid")
    )
    tmpl = (*XY, CORE)
    return jax.shard_map(
        body,
        mesh=finer,
        in_specs=(P(tmpl, "grid", None, None),),
        out_specs=(P(None, "grid", tmpl, None), P("grid", tmpl, None)),
        check_vma=False,
    )
```

```python
import functools
import math

import jax
import jax.numpy as jnp
import numpy as np
from jax import lax
from jax.experimental import pallas as pl
from jax.experimental.pallas import tpu as pltpu
from jax.sharding import Mesh
from jax.sharding import PartitionSpec as P

TOP = 4
SPREAD_FLOOR = 0.25
ROWS = 8
LANES = 128
CHUNKS = (4,) * 8
AHEAD = {0: 6, 1: 8}
FIRST = 3
LIVE = 4
STAT_ORDER = [(c, z) for c in (1, 0) for z in (4, 5, 6, 7, 0, 1, 2, 3)]
CHIP_ORDER = (10, 15, 14, 11, 9, 6, 13, 7, 12, 8, 5, 3, 2, 4, 1, 0)
XY = ("tmpl_0", "tmpl_1")
CORE = "tmpl_2"


def split_table(points):
    order = np.arange(points)
    angle = (order[:, None] * order[None, :] % points) * (2.0 * math.pi / points)
    table = np.concatenate([np.cos(angle), -np.sin(angle)], axis=0)
    mirror = (points - order) % points
    table[:points] = 0.5 * (table[:points] + table[:points][mirror])
    table[points:] = 0.5 * (table[points:] - table[points:][mirror])
    high = table.astype(jnp.bfloat16)
    low = (table - high.astype(np.float64)).astype(jnp.bfloat16)
    pair = [np.kron(np.eye(2), part.astype(np.float64)) for part in (high, low)]
    return np.concatenate(pair, axis=1).astype(jnp.bfloat16)


def diagonal(count, first):
    sub = lax.broadcasted_iota(jnp.int32, (count, LANES), 0)
    lane = lax.broadcasted_iota(jnp.int32, (count, LANES), 1)
    return lane == sub + first


def to_row(column, first):
    return jnp.sum(jnp.where(diagonal(column.shape[0], first), column, 0.0), axis=0, keepdims=True)


def to_column(row, count, first):
    kept = jnp.sum(jnp.where(diagonal(count, first), row, 0.0), axis=1, keepdims=True)
    return jnp.broadcast_to(kept, (count, LANES))


def score_kernel(
    x_hbm, w_hbm, mine_ref, send_ref, stat_ref, x_vmem, w_vmem, plain, square, sems, w_sem
):
    tmpls, slab, beta, doubled = x_vmem.shape
    pairs = beta // 4
    rows = slab * pairs
    core = lax.axis_index(CORE)
    parities = (core, 1 - core)
    outs = (mine_ref, send_ref)

    edges = [sum(CHUNKS[:c]) for c in range(len(CHUNKS) + 1)]
    started = [0]

    def fetch(c):
        block = pl.ds(edges[c], CHUNKS[c])
        return pltpu.make_async_copy(x_hbm.at[block], x_vmem.at[block], sems.at[c])

    def fetch_up_to(c):
        for ahead in range(started[0], c):
            fetch(ahead).start()
        started[0] = max(started[0], c)

    table = pltpu.make_async_copy(w_hbm, w_vmem, w_sem)
    table.start()
    fetch_up_to(FIRST)
    table.wait()

    def parts(t, parity):
        sides = [
            x_vmem[t, :, pl.ds(2 * parity + h, pairs, stride=4), :].reshape(rows, doubled)
            for h in range(2)
        ]
        x = jnp.concatenate(sides, axis=1)
        high = x.astype(jnp.bfloat16)
        rest = x - high.astype(jnp.float32)
        mid = rest.astype(jnp.bfloat16)
        low = (rest - mid.astype(jnp.float32)).astype(jnp.bfloat16)
        return low, mid, high

    def run(*accs):
        first, accs = accs[:2], accs[2:]
        for m in range(2):
            pltpu.matmul_push_rhs(w_vmem[...], staging_register=0, mxu_index=m)
            zeros = jnp.zeros((16, 2 * doubled), jnp.bfloat16)
            pltpu.matmul_acc_lhs(first[m], zeros, load_staged_rhs=0)
            pltpu.matmul_pop(first[m])

        def take(t, u):
            plain_t = square_t = None
            for m in range(2):
                both = pltpu.matmul_pop(accs[2 * u + m])
                s = both[:, :LANES] + both[:, LANES:]
                outs[m][t] = s.reshape(slab, pairs, LANES)
                p = jnp.sum(s.reshape(-1, ROWS, LANES), axis=0)
                q = jnp.sum((s * s).reshape(-1, ROWS, LANES), axis=0)
                plain_t = p if plain_t is None else plain_t + p
                square_t = q if square_t is None else square_t + q
            plain[t] = plain_t
            square[t] = square_t

        for t in range(tmpls):
            if t in edges:
                c = edges.index(t)
                fetch(c).wait()
                fetch_up_to(AHEAD.get(c, 0))
            for m in range(2):
                for part in parts(t, parities[m]):
                    pltpu.matmul_acc_lhs(accs[2 * (t % LIVE) + m], part)
            if t:
                take(t - 1, (t - 1) % LIVE)
        take(tmpls - 1, (tmpls - 1) % LIVE)

    pl.run_scoped(
        run,
        *(pltpu.ACC(m)((16, 256), jnp.float32) for m in range(2)),
        *(pltpu.ACC(m)((rows, 256), jnp.float32) for _ in range(LIVE) for m in range(2)),
    )
    row = 0.0
    for i, part in enumerate((plain, square)):
        whole = jnp.sum(part[...], axis=1)
        row = row + to_row(jnp.sum(whole, axis=1, keepdims=True), i * tmpls)
    stat_ref[...] = jnp.broadcast_to(row[None], stat_ref.shape)


def order(a, b):
    return jnp.maximum(a, b), jnp.minimum(a, b)


def sort4(a, b, c, d):
    a, b = order(a, b)
    c, d = order(c, d)
    a, c = order(a, c)
    b, d = order(b, d)
    b, c = order(b, c)
    return a, b, c, d


def merge4(u, v):
    a, b, c, d = (jnp.maximum(u[i], v[3 - i]) for i in range(4))
    a, c = order(a, c)
    b, d = order(b, d)
    a, b = order(a, b)
    c, d = order(c, d)
    return a, b, c, d


def top_kernel(count, mine_ref, other_ref, stat_ref, out_ref, gain_ref, shift_ref, staged):
    tmpls, slab, pairs, _ = mine_ref.shape
    for half in range(2):
        total = sum(stat_ref[p] for p, (c, _) in enumerate(STAT_ORDER) if c == half)
        average = to_column(total, tmpls, 0) / count
        spread = to_column(total, tmpls, tmpls) / count - average * average
        gain_ref[pl.ds(half * tmpls, tmpls)] = 1.0 / jnp.sqrt(spread + SPREAD_FLOOR)
        shift_ref[pl.ds(half * tmpls, tmpls)] = average
    core = lax.axis_index(CORE)
    firsts = (core * tmpls, (1 - core) * tmpls)

    def tile(a, carry):
        for q in range(pairs // ROWS):
            best = total = None
            for first, ref in zip(firsts, (mine_ref, other_ref)):
                for group in range(tmpls // 4):
                    four = []
                    for t in range(4 * group, 4 * group + 4):
                        s = ref[t, a, pl.ds(q * ROWS, ROWS)]
                        g = gain_ref[pl.ds(first + t, ROWS, stride=0)]
                        m = shift_ref[pl.ds(first + t, ROWS, stride=0)]
                        four.append((s - m) * g)
                    part = (four[0] + four[1]) + (four[2] + four[3])
                    total = part if total is None else total + part
                    four = sort4(*four)
                    best = four if best is None else merge4(best, four)
            for r, value in enumerate((*best, total)):
                start = (q * ROWS * (TOP + 1) + r) * slab + a
                staged[pl.ds(start, ROWS, stride=(TOP + 1) * slab)] = value
        return carry

    lax.fori_loop(0, slab, tile, 0)
    size = (TOP + 1) * slab
    for place, chip in enumerate(CHIP_ORDER):
        out_ref[place * size : (place + 1) * size] = staged[chip * size : (chip + 1) * size]


def final_kernel(norm, in_ref, best_ref, sum_ref):
    peers = in_ref.shape[0]
    points = best_ref.shape[-1]
    fours = [tuple(in_ref[p, r] for r in range(TOP)) for p in range(peers)]
    total = in_ref[0, TOP]
    for p in range(1, peers):
        total = total + in_ref[p, TOP]
    while len(fours) > 1:
        fours = [merge4(u, v) for u, v in zip(fours[::2], fours[1::2])]
    total = total / norm
    for h in range(2):
        lanes = slice(h * points, (h + 1) * points)
        for r in range(TOP):
            best_ref[r, :, h, :] = fours[0][r][:, lanes]
        sum_ref[:, h, :] = total[:, lanes]


def body(spectrum):
    tmpls, slab, beta, doubled = spectrum.shape
    points = doubled // 2
    pairs = beta // 4
    chips = lax.axis_size(XY)
    peers = 2 * lax.axis_size("grid")
    vmem = pl.BlockSpec(memory_space=pltpu.VMEM)
    part = jax.ShapeDtypeStruct((tmpls, slab, pairs, LANES), jnp.float32)
    mine, send, stat = pl.pallas_call(
        score_kernel,
        out_shape=(part, part, jax.ShapeDtypeStruct((peers, 1, LANES), jnp.float32)),
        in_specs=[pl.BlockSpec(memory_space=pltpu.HBM)] * 2,
        out_specs=(vmem, vmem, vmem),
        scratch_shapes=[
            pltpu.VMEM(spectrum.shape, jnp.float32),
            pltpu.VMEM((2 * doubled, 2 * doubled), jnp.bfloat16),
            pltpu.VMEM((tmpls, ROWS, LANES), jnp.float32),
            pltpu.VMEM((tmpls, ROWS, LANES), jnp.float32),
            pltpu.SemaphoreType.DMA((len(CHUNKS),)),
            pltpu.SemaphoreType.DMA,
        ],
        compiler_params=pltpu.CompilerParams(vmem_limit_bytes=40 * 2**20),
        name="scores",
    )(*(
        pltpu.with_memory_space_constraint(a, pltpu.HBM)
        for a in (spectrum, jnp.asarray(split_table(points)))
    ))
    meeting = [[c * lax.axis_size("grid") + z for c, z in STAT_ORDER]]
    stats = lax.all_to_all(
        stat, (CORE, "grid"), split_axis=0, concat_axis=0, axis_index_groups=meeting, tiled=True
    )
    other = lax.ppermute(send, CORE, [(0, 1), (1, 0)])
    packed = pl.pallas_call(
        functools.partial(top_kernel, float(points**3)),
        out_shape=jax.ShapeDtypeStruct((chips * (TOP + 1) * slab, LANES), jnp.float32),
        in_specs=[vmem, vmem, vmem],
        out_specs=vmem,
        scratch_shapes=[
            pltpu.VMEM((2 * tmpls, LANES), jnp.float32),
            pltpu.VMEM((2 * tmpls, LANES), jnp.float32),
            pltpu.VMEM((chips * (TOP + 1) * slab, LANES), jnp.float32),
        ],
        compiler_params=pltpu.CompilerParams(vmem_limit_bytes=20 * 2**20),
        name="tops",
    )(mine, other, stats)
    packed = packed.reshape(chips, TOP + 1, slab, LANES)
    received = lax.all_to_all(
        packed, XY, split_axis=0, concat_axis=0, axis_index_groups=[list(CHIP_ORDER)], tiled=True
    )
    return pl.pallas_call(
        functools.partial(final_kernel, math.sqrt(2 * chips * tmpls)),
        out_shape=(
            jax.ShapeDtypeStruct((TOP, slab, 2, points), jnp.float32),
            jax.ShapeDtypeStruct((slab, 2, points), jnp.float32),
        ),
        in_specs=[vmem],
        out_specs=(vmem, vmem),
        compiler_params=pltpu.CompilerParams(vmem_limit_bytes=8 * 2**20),
        name="finish",
    )(received)


def solution(mesh):
    finer = Mesh(
        mesh.devices.reshape(4, 4, 2, mesh.shape["grid"]), (*XY, CORE, "grid")
    )
    tmpl = (*XY, CORE)
    return jax.shard_map(
        body,
        mesh=finer,
        in_specs=(P(tmpl, "grid", None, None),),
        out_specs=(P(None, "grid", tmpl, None), P("grid", tmpl, None)),
        check_vma=False,
    )
```

```python
import functools
import math

import jax
import jax.numpy as jnp
import numpy as np
from jax import lax
from jax.experimental import pallas as pl
from jax.experimental.pallas import tpu as pltpu
from jax.sharding import Mesh
from jax.sharding import PartitionSpec as P

TOP = 4
SPREAD_FLOOR = 0.25
ROWS = 8
LANES = 128
CHUNKS = (4,) * 8
AHEAD = {0: 6, 1: 8}
FIRST = 3
LIVE = 4
CORE_ORDER = (1, 0)
GRID_ORDER = (4, 5, 6, 7, 0, 1, 2, 3)
CHIP_ORDER = (10, 15, 14, 11, 9, 6, 13, 7, 12, 8, 5, 3, 2, 4, 1, 0)
XY = ("tmpl_0", "tmpl_1")
CORE = "tmpl_2"


def split_table(points):
    order = np.arange(points)
    angle = (order[:, None] * order[None, :] % points) * (2.0 * math.pi / points)
    table = np.concatenate([np.cos(angle), -np.sin(angle)], axis=0)
    mirror = (points - order) % points
    table[:points] = 0.5 * (table[:points] + table[:points][mirror])
    table[points:] = 0.5 * (table[points:] - table[points:][mirror])
    high = table.astype(jnp.bfloat16)
    low = (table - high.astype(np.float64)).astype(jnp.bfloat16)
    pair = [np.kron(np.eye(2), part.astype(np.float64)) for part in (high, low)]
    return np.concatenate(pair, axis=1).astype(jnp.bfloat16)


def diagonal(count, first):
    sub = lax.broadcasted_iota(jnp.int32, (count, LANES), 0)
    lane = lax.broadcasted_iota(jnp.int32, (count, LANES), 1)
    return lane == sub + first


def to_row(column, first):
    return jnp.sum(jnp.where(diagonal(column.shape[0], first), column, 0.0), axis=0, keepdims=True)


def to_column(row, count):
    kept = jnp.sum(jnp.where(diagonal(count, 0), row, 0.0), axis=1, keepdims=True)
    return jnp.broadcast_to(kept, (count, LANES))


def score_kernel(
    x_hbm, w_hbm, mine_ref, send_ref, stat_ref, x_vmem, w_vmem, plain, square, bases, sems, w_sem
):
    tmpls, slab, beta, doubled = x_vmem.shape
    pairs = beta // 4
    rows = slab * pairs
    core = lax.axis_index(CORE)
    parities = (core, 1 - core)
    outs = (mine_ref, send_ref)

    edges = [sum(CHUNKS[:c]) for c in range(len(CHUNKS) + 1)]
    started = [0]

    def fetch(c):
        block = pl.ds(edges[c], CHUNKS[c])
        return pltpu.make_async_copy(x_hbm.at[block], x_vmem.at[block], sems.at[c])

    def fetch_up_to(c):
        for ahead in range(started[0], c):
            fetch(ahead).start()
        started[0] = max(started[0], c)

    table = pltpu.make_async_copy(w_hbm, w_vmem, w_sem)
    table.start()
    fetch_up_to(FIRST)
    table.wait()

    def base_of(t):
        some = x_vmem[t, : slab // 4].reshape(-1, ROWS, LANES)
        mean = jnp.sum(jnp.sum(some, axis=0), axis=0, keepdims=True) / (slab // 4 * beta)
        lane = lax.broadcasted_iota(jnp.int32, (1, LANES), 1)
        base = jnp.where(lane == 0, mean, 0.0)
        bases[pl.ds(t, 1)] = base
        return base

    def parts(t, parity, base):
        sides = [
            x_vmem[t, :, pl.ds(2 * parity + h, pairs, stride=4), :].reshape(rows, doubled) - base
            for h in range(2)
        ]
        x = jnp.concatenate(sides, axis=1)
        high = x.astype(jnp.bfloat16)
        return (x - high.astype(jnp.float32)).astype(jnp.bfloat16), high

    def run(*accs):
        first, accs = accs[:2], accs[2:]
        for m in range(2):
            pltpu.matmul_push_rhs(w_vmem[...], staging_register=0, mxu_index=m)
            zeros = jnp.zeros((16, 2 * doubled), jnp.bfloat16)
            pltpu.matmul_acc_lhs(first[m], zeros, load_staged_rhs=0)
            pltpu.matmul_pop(first[m])

        def take(t, u):
            plain_t = square_t = None
            for m in range(2):
                both = pltpu.matmul_pop(accs[2 * u + m])
                s = both[:, :LANES] + both[:, LANES:]
                outs[m][t] = s.reshape(slab, pairs, LANES)
                p = jnp.sum(s.reshape(-1, ROWS, LANES), axis=0)
                q = jnp.sum((s * s).reshape(-1, ROWS, LANES), axis=0)
                plain_t = p if plain_t is None else plain_t + p
                square_t = q if square_t is None else square_t + q
            plain[t] = plain_t
            square[t] = square_t

        for t in range(tmpls):
            if t in edges:
                c = edges.index(t)
                fetch(c).wait()
                fetch_up_to(AHEAD.get(c, 0))
            base = base_of(t)
            for m in range(2):
                for part in parts(t, parities[m], base):
                    pltpu.matmul_acc_lhs(accs[2 * (t % LIVE) + m], part)
            if t:
                take(t - 1, (t - 1) % LIVE)
        take(tmpls - 1, (tmpls - 1) % LIVE)

    pl.run_scoped(
        run,
        *(pltpu.ACC(m)((16, 256), jnp.float32) for m in range(2)),
        *(pltpu.ACC(m)((rows, 256), jnp.float32) for _ in range(LIVE) for m in range(2)),
    )
    row = 0.0
    for i, part in enumerate((jnp.sum(plain[...], axis=1), jnp.sum(square[...], axis=1), bases[...])):
        row = row + to_row(jnp.sum(part, axis=1, keepdims=True), i * tmpls)
    stat_ref[...] = jnp.broadcast_to(row[None], stat_ref.shape)


def order(a, b):
    return jnp.maximum(a, b), jnp.minimum(a, b)


def sort4(a, b, c, d):
    a, b = order(a, b)
    c, d = order(c, d)
    a, c = order(a, c)
    b, d = order(b, d)
    b, c = order(b, c)
    return a, b, c, d


def merge4(u, v):
    a, b, c, d = (jnp.maximum(u[i], v[3 - i]) for i in range(4))
    a, c = order(a, c)
    b, d = order(b, d)
    a, b = order(a, b)
    c, d = order(c, d)
    return a, b, c, d


def top_kernel(count, mine_ref, other_ref, stat_ref, out_ref, gain_ref, shift_ref, staged):
    tmpls, slab, pairs, _ = mine_ref.shape
    peers = stat_ref.shape[0]
    slabs = peers // 2
    rows = stat_ref[...].reshape(peers, LANES)
    turned = [rows] + [pltpu.roll(rows, LANES - i * tmpls, 1) for i in (1, 2)]
    sub = lax.broadcasted_iota(jnp.int32, (slabs, LANES), 0)
    here = sum(jnp.where(lax.axis_index("grid") == z, i, 0) for i, z in enumerate(GRID_ORDER))
    for place, half in enumerate(CORE_ORDER):
        plain, square, base = (v[place * slabs : (place + 1) * slabs] for v in turned)
        average = jnp.sum(plain / count + base / slabs, axis=0, keepdims=True)
        off = average - base
        spread = square - 2.0 * off * plain + (count / slabs) * (off * off)
        spread = jnp.sum(spread, axis=0, keepdims=True) / count
        gain = 1.0 / jnp.sqrt(spread + SPREAD_FLOOR)
        shift = jnp.sum(jnp.where(sub == here, off, 0.0), axis=0, keepdims=True)
        gain_ref[pl.ds(half * tmpls, tmpls)] = to_column(gain, tmpls)
        shift_ref[pl.ds(half * tmpls, tmpls)] = to_column(shift, tmpls)
    core = lax.axis_index(CORE)
    firsts = (core * tmpls, (1 - core) * tmpls)

    def tile(a, carry):
        for q in range(pairs // ROWS):
            best = total = None
            for first, ref in zip(firsts, (mine_ref, other_ref)):
                for group in range(tmpls // 4):
                    four = []
                    for t in range(4 * group, 4 * group + 4):
                        s = ref[t, a, pl.ds(q * ROWS, ROWS)]
                        g = gain_ref[pl.ds(first + t, ROWS, stride=0)]
                        m = shift_ref[pl.ds(first + t, ROWS, stride=0)]
                        four.append((s - m) * g)
                    part = (four[0] + four[1]) + (four[2] + four[3])
                    total = part if total is None else total + part
                    four = sort4(*four)
                    best = four if best is None else merge4(best, four)
            for r, value in enumerate((*best, total)):
                start = (q * ROWS * (TOP + 1) + r) * slab + a
                staged[pl.ds(start, ROWS, stride=(TOP + 1) * slab)] = value
        return carry

    lax.fori_loop(0, slab, tile, 0)
    size = (TOP + 1) * slab
    for place, chip in enumerate(CHIP_ORDER):
        out_ref[place * size : (place + 1) * size] = staged[chip * size : (chip + 1) * size]


def final_kernel(norm, in_ref, best_ref, sum_ref):
    peers = in_ref.shape[0]
    points = best_ref.shape[-1]
    fours = [tuple(in_ref[p, r] for r in range(TOP)) for p in range(peers)]
    total = in_ref[0, TOP]
    for p in range(1, peers):
        total = total + in_ref[p, TOP]
    while len(fours) > 1:
        fours = [merge4(u, v) for u, v in zip(fours[::2], fours[1::2])]
    total = total / norm
    for h in range(2):
        lanes = slice(h * points, (h + 1) * points)
        for r in range(TOP):
            best_ref[r, :, h, :] = fours[0][r][:, lanes]
        sum_ref[:, h, :] = total[:, lanes]


def body(spectrum):
    tmpls, slab, beta, doubled = spectrum.shape
    points = doubled // 2
    pairs = beta // 4
    chips = lax.axis_size(XY)
    peers = 2 * lax.axis_size("grid")
    vmem = pl.BlockSpec(memory_space=pltpu.VMEM)
    part = jax.ShapeDtypeStruct((tmpls, slab, pairs, LANES), jnp.float32)
    mine, send, stat = pl.pallas_call(
        score_kernel,
        out_shape=(part, part, jax.ShapeDtypeStruct((peers, 1, LANES), jnp.float32)),
        in_specs=[pl.BlockSpec(memory_space=pltpu.HBM)] * 2,
        out_specs=(vmem, vmem, vmem),
        scratch_shapes=[
            pltpu.VMEM(spectrum.shape, jnp.float32),
            pltpu.VMEM((2 * doubled, 2 * doubled), jnp.bfloat16),
            pltpu.VMEM((tmpls, ROWS, LANES), jnp.float32),
            pltpu.VMEM((tmpls, ROWS, LANES), jnp.float32),
            pltpu.VMEM((tmpls, LANES), jnp.float32),
            pltpu.SemaphoreType.DMA((len(CHUNKS),)),
            pltpu.SemaphoreType.DMA,
        ],
        compiler_params=pltpu.CompilerParams(vmem_limit_bytes=40 * 2**20),
        name="scores",
    )(*(
        pltpu.with_memory_space_constraint(a, pltpu.HBM)
        for a in (spectrum, jnp.asarray(split_table(points)))
    ))
    meeting = [[c * lax.axis_size("grid") + z for c in CORE_ORDER for z in GRID_ORDER]]
    stats = lax.all_to_all(
        stat, (CORE, "grid"), split_axis=0, concat_axis=0, axis_index_groups=meeting, tiled=True
    )
    other = lax.ppermute(send, CORE, [(0, 1), (1, 0)])
    packed = pl.pallas_call(
        functools.partial(top_kernel, float(points**3)),
        out_shape=jax.ShapeDtypeStruct((chips * (TOP + 1) * slab, LANES), jnp.float32),
        in_specs=[vmem, vmem, vmem],
        out_specs=vmem,
        scratch_shapes=[
            pltpu.VMEM((2 * tmpls, LANES), jnp.float32),
            pltpu.VMEM((2 * tmpls, LANES), jnp.float32),
            pltpu.VMEM((chips * (TOP + 1) * slab, LANES), jnp.float32),
        ],
        compiler_params=pltpu.CompilerParams(vmem_limit_bytes=20 * 2**20),
        name="tops",
    )(mine, other, stats)
    packed = packed.reshape(chips, TOP + 1, slab, LANES)
    received = lax.all_to_all(
        packed, XY, split_axis=0, concat_axis=0, axis_index_groups=[list(CHIP_ORDER)], tiled=True
    )
    return pl.pallas_call(
        functools.partial(final_kernel, math.sqrt(2 * chips * tmpls)),
        out_shape=(
            jax.ShapeDtypeStruct((TOP, slab, 2, points), jnp.float32),
            jax.ShapeDtypeStruct((slab, 2, points), jnp.float32),
        ),
        in_specs=[vmem],
        out_specs=(vmem, vmem),
        compiler_params=pltpu.CompilerParams(vmem_limit_bytes=8 * 2**20),
        name="finish",
    )(received)


def solution(mesh):
    finer = Mesh(
        mesh.devices.reshape(4, 4, 2, mesh.shape["grid"]), (*XY, CORE, "grid")
    )
    tmpl = (*XY, CORE)
    return jax.shard_map(
        body,
        mesh=finer,
        in_specs=(P(tmpl, "grid", None, None),),
        out_specs=(P(None, "grid", tmpl, None), P("grid", tmpl, None)),
        check_vma=False,
    )
```

```python
import functools
import math

import jax
import jax.numpy as jnp
import numpy as np
from jax import lax
from jax.experimental import pallas as pl
from jax.experimental.pallas import tpu as pltpu
from jax.sharding import Mesh
from jax.sharding import PartitionSpec as P

TOP = 4
SPREAD_FLOOR = 0.25
ROWS = 8
LANES = 128
CHUNKS = (2, 2, 4, 8, 8, 8)
AHEAD = {0: 5, 1: 6}
FIRST = 4
LIVE = 4
STAT_ORDER = [(c, z) for c in (1, 0) for z in (4, 5, 6, 7, 0, 1, 2, 3)]
CHIP_ORDER = (10, 15, 14, 11, 9, 6, 13, 7, 12, 8, 5, 3, 2, 4, 1, 0)
XY = ("tmpl_0", "tmpl_1")
CORE = "tmpl_2"


def split_table(points):
    order = np.arange(points)
    angle = (order[:, None] * order[None, :] % points) * (2.0 * math.pi / points)
    table = np.concatenate([np.cos(angle), -np.sin(angle)], axis=0)
    mirror = (points - order) % points
    table[:points] = 0.5 * (table[:points] + table[:points][mirror])
    table[points:] = 0.5 * (table[points:] - table[points:][mirror])
    high = table.astype(jnp.bfloat16)
    low = (table - high.astype(np.float64)).astype(jnp.bfloat16)
    pair = [np.kron(np.eye(2), part.astype(np.float64)) for part in (high, low)]
    return np.concatenate(pair, axis=1).astype(jnp.bfloat16)


def diagonal(count, first):
    sub = lax.broadcasted_iota(jnp.int32, (count, LANES), 0)
    lane = lax.broadcasted_iota(jnp.int32, (count, LANES), 1)
    return lane == sub + first


def to_row(column, first):
    return jnp.sum(jnp.where(diagonal(column.shape[0], first), column, 0.0), axis=0, keepdims=True)


def to_column(row, count, first):
    kept = jnp.sum(jnp.where(diagonal(count, first), row, 0.0), axis=1, keepdims=True)
    return jnp.broadcast_to(kept, (count, LANES))


def score_kernel(
    x_hbm, w_hbm, mine_ref, send_ref, stat_ref, x_vmem, w_vmem, plain, square, sems, w_sem
):
    tmpls, slab, beta, doubled = x_vmem.shape
    pairs = beta // 4
    rows = slab * pairs
    core = lax.axis_index(CORE)
    parities = (core, 1 - core)
    outs = (mine_ref, send_ref)

    edges = [sum(CHUNKS[:c]) for c in range(len(CHUNKS) + 1)]
    started = [0]

    def fetch(c):
        block = pl.ds(edges[c], CHUNKS[c])
        return pltpu.make_async_copy(x_hbm.at[block], x_vmem.at[block], sems.at[c])

    def fetch_up_to(c):
        for ahead in range(started[0], c):
            fetch(ahead).start()
        started[0] = max(started[0], c)

    table = pltpu.make_async_copy(w_hbm, w_vmem, w_sem)
    table.start()
    fetch_up_to(FIRST)
    table.wait()

    def parts(t, parity):
        sides = [
            x_vmem[t, :, pl.ds(2 * parity + h, pairs, stride=4), :].reshape(rows, doubled)
            for h in range(2)
        ]
        x = jnp.concatenate(sides, axis=1)
        high = x.astype(jnp.bfloat16)
        rest = x - high.astype(jnp.float32)
        mid = rest.astype(jnp.bfloat16)
        low = (rest - mid.astype(jnp.float32)).astype(jnp.bfloat16)
        return low, mid, high

    def run(*accs):
        first, accs = accs[:2], accs[2:]
        for m in range(2):
            pltpu.matmul_push_rhs(w_vmem[...], staging_register=0, mxu_index=m)
            zeros = jnp.zeros((16, 2 * doubled), jnp.bfloat16)
            pltpu.matmul_acc_lhs(first[m], zeros, load_staged_rhs=0)
            pltpu.matmul_pop(first[m])

        def take(t, u):
            plain_t = square_t = None
            for m in range(2):
                both = pltpu.matmul_pop(accs[2 * u + m])
                s = both[:, :LANES] + both[:, LANES:]
                outs[m][t] = s.reshape(slab, pairs, LANES)
                p = jnp.sum(s.reshape(-1, ROWS, LANES), axis=0)
                q = jnp.sum((s * s).reshape(-1, ROWS, LANES), axis=0)
                plain_t = p if plain_t is None else plain_t + p
                square_t = q if square_t is None else square_t + q
            plain[t] = plain_t
            square[t] = square_t

        for t in range(tmpls):
            if t in edges:
                c = edges.index(t)
                fetch(c).wait()
                fetch_up_to(AHEAD.get(c, 0))
            for m in range(2):
                for part in parts(t, parities[m]):
                    pltpu.matmul_acc_lhs(accs[2 * (t % LIVE) + m], part)
            if t:
                take(t - 1, (t - 1) % LIVE)
        take(tmpls - 1, (tmpls - 1) % LIVE)

    pl.run_scoped(
        run,
        *(pltpu.ACC(m)((16, 256), jnp.float32) for m in range(2)),
        *(pltpu.ACC(m)((rows, 256), jnp.float32) for _ in range(LIVE) for m in range(2)),
    )
    row = 0.0
    for i, part in enumerate((plain, square)):
        whole = jnp.sum(part[...], axis=1)
        row = row + to_row(jnp.sum(whole, axis=1, keepdims=True), i * tmpls)
    stat_ref[...] = jnp.broadcast_to(row[None], stat_ref.shape)


def order(a, b):
    return jnp.maximum(a, b), jnp.minimum(a, b)


def sort4(a, b, c, d):
    a, b = order(a, b)
    c, d = order(c, d)
    a, c = order(a, c)
    b, d = order(b, d)
    b, c = order(b, c)
    return a, b, c, d


def merge4(u, v):
    a, b, c, d = (jnp.maximum(u[i], v[3 - i]) for i in range(4))
    a, c = order(a, c)
    b, d = order(b, d)
    a, b = order(a, b)
    c, d = order(c, d)
    return a, b, c, d


def top_kernel(count, mine_ref, other_ref, stat_ref, out_ref, gain_ref, shift_ref, staged):
    tmpls, slab, pairs, _ = mine_ref.shape
    for half in range(2):
        total = sum(stat_ref[p] for p, (c, _) in enumerate(STAT_ORDER) if c == half)
        average = to_column(total, tmpls, 0) / count
        spread = to_column(total, tmpls, tmpls) / count - average * average
        gain_ref[pl.ds(half * tmpls, tmpls)] = 1.0 / jnp.sqrt(spread + SPREAD_FLOOR)
        shift_ref[pl.ds(half * tmpls, tmpls)] = average
    core = lax.axis_index(CORE)
    firsts = (core * tmpls, (1 - core) * tmpls)

    def tile(a, carry):
        for q in range(pairs // ROWS):
            best = total = None
            for first, ref in zip(firsts, (mine_ref, other_ref)):
                for group in range(tmpls // 4):
                    four = []
                    for t in range(4 * group, 4 * group + 4):
                        s = ref[t, a, pl.ds(q * ROWS, ROWS)]
                        g = gain_ref[pl.ds(first + t, ROWS, stride=0)]
                        m = shift_ref[pl.ds(first + t, ROWS, stride=0)]
                        four.append((s - m) * g)
                    part = (four[0] + four[1]) + (four[2] + four[3])
                    total = part if total is None else total + part
                    four = sort4(*four)
                    best = four if best is None else merge4(best, four)
            for r, value in enumerate((*best, total)):
                start = (q * ROWS * (TOP + 1) + r) * slab + a
                staged[pl.ds(start, ROWS, stride=(TOP + 1) * slab)] = value
        return carry

    lax.fori_loop(0, slab, tile, 0)
    size = (TOP + 1) * slab
    for place, chip in enumerate(CHIP_ORDER):
        out_ref[place * size : (place + 1) * size] = staged[chip * size : (chip + 1) * size]


def final_kernel(norm, in_ref, best_ref, sum_ref):
    peers = in_ref.shape[0]
    points = best_ref.shape[-1]
    fours = [tuple(in_ref[p, r] for r in range(TOP)) for p in range(peers)]
    total = in_ref[0, TOP]
    for p in range(1, peers):
        total = total + in_ref[p, TOP]
    while len(fours) > 1:
        fours = [merge4(u, v) for u, v in zip(fours[::2], fours[1::2])]
    total = total / norm
    for h in range(2):
        lanes = slice(h * points, (h + 1) * points)
        for r in range(TOP):
            best_ref[r, :, h, :] = fours[0][r][:, lanes]
        sum_ref[:, h, :] = total[:, lanes]


def body(spectrum):
    tmpls, slab, beta, doubled = spectrum.shape
    points = doubled // 2
    pairs = beta // 4
    chips = lax.axis_size(XY)
    peers = 2 * lax.axis_size("grid")
    vmem = pl.BlockSpec(memory_space=pltpu.VMEM)
    part = jax.ShapeDtypeStruct((tmpls, slab, pairs, LANES), jnp.float32)
    mine, send, stat = pl.pallas_call(
        score_kernel,
        out_shape=(part, part, jax.ShapeDtypeStruct((peers, 1, LANES), jnp.float32)),
        in_specs=[pl.BlockSpec(memory_space=pltpu.HBM)] * 2,
        out_specs=(vmem, vmem, vmem),
        scratch_shapes=[
            pltpu.VMEM(spectrum.shape, jnp.float32),
            pltpu.VMEM((2 * doubled, 2 * doubled), jnp.bfloat16),
            pltpu.VMEM((tmpls, ROWS, LANES), jnp.float32),
            pltpu.VMEM((tmpls, ROWS, LANES), jnp.float32),
            pltpu.SemaphoreType.DMA((len(CHUNKS),)),
            pltpu.SemaphoreType.DMA,
        ],
        compiler_params=pltpu.CompilerParams(vmem_limit_bytes=40 * 2**20),
        name="scores",
    )(*(
        pltpu.with_memory_space_constraint(a, pltpu.HBM)
        for a in (spectrum, jnp.asarray(split_table(points)))
    ))
    meeting = [[c * lax.axis_size("grid") + z for c, z in STAT_ORDER]]
    stats = lax.all_to_all(
        stat, (CORE, "grid"), split_axis=0, concat_axis=0, axis_index_groups=meeting, tiled=True
    )
    other = lax.ppermute(send, CORE, [(0, 1), (1, 0)])
    packed = pl.pallas_call(
        functools.partial(top_kernel, float(points**3)),
        out_shape=jax.ShapeDtypeStruct((chips * (TOP + 1) * slab, LANES), jnp.float32),
        in_specs=[vmem, vmem, vmem],
        out_specs=vmem,
        scratch_shapes=[
            pltpu.VMEM((2 * tmpls, LANES), jnp.float32),
            pltpu.VMEM((2 * tmpls, LANES), jnp.float32),
            pltpu.VMEM((chips * (TOP + 1) * slab, LANES), jnp.float32),
        ],
        compiler_params=pltpu.CompilerParams(vmem_limit_bytes=20 * 2**20),
        name="tops",
    )(mine, other, stats)
    packed = packed.reshape(chips, TOP + 1, slab, LANES)
    received = lax.all_to_all(
        packed, XY, split_axis=0, concat_axis=0, axis_index_groups=[list(CHIP_ORDER)], tiled=True
    )
    return pl.pallas_call(
        functools.partial(final_kernel, math.sqrt(2 * chips * tmpls)),
        out_shape=(
            jax.ShapeDtypeStruct((TOP, slab, 2, points), jnp.float32),
            jax.ShapeDtypeStruct((slab, 2, points), jnp.float32),
        ),
        in_specs=[vmem],
        out_specs=(vmem, vmem),
        compiler_params=pltpu.CompilerParams(vmem_limit_bytes=8 * 2**20),
        name="finish",
    )(received)


def solution(mesh):
    finer = Mesh(
        mesh.devices.reshape(4, 4, 2, mesh.shape["grid"]), (*XY, CORE, "grid")
    )
    tmpl = (*XY, CORE)
    return jax.shard_map(
        body,
        mesh=finer,
        in_specs=(P(tmpl, "grid", None, None),),
        out_specs=(P(None, "grid", tmpl, None), P("grid", tmpl, None)),
        check_vma=False,
    )
```

```python
import functools
import math

import jax
import jax.numpy as jnp
import numpy as np
from jax import lax
from jax.experimental import pallas as pl
from jax.experimental.pallas import tpu as pltpu
from jax.sharding import Mesh
from jax.sharding import PartitionSpec as P

TOP = 4
SPREAD_FLOOR = 0.25
ROWS = 8
LANES = 128
CHUNKS = (2, 2, 4, 8, 8, 8)
AHEAD = {0: 5, 1: 6}
FIRST = 4
LIVE = 4
STAT_ORDER = [(c, z) for c in (1, 0) for z in (4, 5, 6, 7, 0, 1, 2, 3)]
CHIP_ORDER = (10, 15, 14, 11, 9, 6, 13, 7, 12, 8, 5, 3, 2, 4, 1, 0)
XY = ("tmpl_0", "tmpl_1")
CORE = "tmpl_2"


def split_table(points):
    order = np.arange(points)
    angle = (order[:, None] * order[None, :] % points) * (2.0 * math.pi / points)
    table = np.concatenate([np.cos(angle), -np.sin(angle)], axis=0)
    mirror = (points - order) % points
    table[:points] = 0.5 * (table[:points] + table[:points][mirror])
    table[points:] = 0.5 * (table[points:] - table[points:][mirror])
    high = table.astype(jnp.bfloat16)
    low = (table - high.astype(np.float64)).astype(jnp.bfloat16)
    pair = [np.kron(np.eye(2), part.astype(np.float64)) for part in (high, low)]
    return np.concatenate(pair, axis=1).astype(jnp.bfloat16)


def diagonal(count, first):
    sub = lax.broadcasted_iota(jnp.int32, (count, LANES), 0)
    lane = lax.broadcasted_iota(jnp.int32, (count, LANES), 1)
    return lane == sub + first


def to_row(column, first):
    return jnp.sum(jnp.where(diagonal(column.shape[0], first), column, 0.0), axis=0, keepdims=True)


def to_column(row, count, first):
    kept = jnp.sum(jnp.where(diagonal(count, first), row, 0.0), axis=1, keepdims=True)
    return jnp.broadcast_to(kept, (count, LANES))


def score_kernel(
    x_hbm, w_hbm, mine_ref, send_ref, stat_ref, x_vmem, w_vmem, plain, square, sems, w_sem
):
    tmpls, slab, beta, doubled = x_vmem.shape
    pairs = beta // 4
    rows = slab * pairs
    core = lax.axis_index(CORE)
    parities = (core, 1 - core)
    outs = (mine_ref, send_ref)

    edges = [sum(CHUNKS[:c]) for c in range(len(CHUNKS) + 1)]
    started = [0]

    def fetch(c):
        block = pl.ds(edges[c], CHUNKS[c])
        return pltpu.make_async_copy(x_hbm.at[block], x_vmem.at[block], sems.at[c])

    def fetch_up_to(c):
        for ahead in range(started[0], c):
            fetch(ahead).start()
        started[0] = max(started[0], c)

    table = pltpu.make_async_copy(w_hbm, w_vmem, w_sem)
    table.start()
    fetch_up_to(FIRST)
    table.wait()

    def parts(t, parity):
        sides = [
            x_vmem[t, :, pl.ds(2 * parity + h, pairs, stride=4), :].reshape(rows, doubled)
            for h in range(2)
        ]
        x = jnp.concatenate(sides, axis=1)
        high = x.astype(jnp.bfloat16)
        rest = x - high.astype(jnp.float32)
        mid = rest.astype(jnp.bfloat16)
        low = (rest - mid.astype(jnp.float32)).astype(jnp.bfloat16)
        return low, mid, high

    def run(*accs):
        first, accs = accs[:2], accs[2:]
        for m in range(2):
            pltpu.matmul_push_rhs(w_vmem[...], staging_register=0, mxu_index=m)
            zeros = jnp.zeros((16, 2 * doubled), jnp.bfloat16)
            pltpu.matmul_acc_lhs(first[m], zeros, load_staged_rhs=0)
            pltpu.matmul_pop(first[m])

        def take(t, u):
            plain_t = square_t = None
            for m in range(2):
                both = pltpu.matmul_pop(accs[2 * u + m])
                s = both[:, :LANES] + both[:, LANES:]
                outs[m][t] = s.reshape(slab, pairs, LANES)
                p = jnp.sum(s.reshape(-1, ROWS, LANES), axis=0)
                q = jnp.sum((s * s).reshape(-1, ROWS, LANES), axis=0)
                plain_t = p if plain_t is None else plain_t + p
                square_t = q if square_t is None else square_t + q
            plain[t] = plain_t
            square[t] = square_t

        for t in range(tmpls):
            if t in edges:
                c = edges.index(t)
                fetch(c).wait()
                fetch_up_to(AHEAD.get(c, 0))
            for m in range(2):
                for part in parts(t, parities[m]):
                    pltpu.matmul_acc_lhs(accs[2 * (t % LIVE) + m], part)
            if t:
                take(t - 1, (t - 1) % LIVE)
        take(tmpls - 1, (tmpls - 1) % LIVE)

    pl.run_scoped(
        run,
        *(pltpu.ACC(m)((16, 256), jnp.float32) for m in range(2)),
        *(pltpu.ACC(m)((rows, 256), jnp.float32) for _ in range(LIVE) for m in range(2)),
    )
    row = 0.0
    for i, part in enumerate((plain, square)):
        whole = jnp.sum(part[...], axis=1)
        row = row + to_row(jnp.sum(whole, axis=1, keepdims=True), i * tmpls)
    stat_ref[...] = jnp.broadcast_to(row[None], stat_ref.shape)


def order(a, b):
    return jnp.maximum(a, b), jnp.minimum(a, b)


def sort4(a, b, c, d):
    a, b = order(a, b)
    c, d = order(c, d)
    a, c = order(a, c)
    b, d = order(b, d)
    b, c = order(b, c)
    return a, b, c, d


def merge4(u, v):
    a, b, c, d = (jnp.maximum(u[i], v[3 - i]) for i in range(4))
    a, c = order(a, c)
    b, d = order(b, d)
    a, b = order(a, b)
    c, d = order(c, d)
    return a, b, c, d


def top_kernel(count, mine_ref, other_ref, stat_ref, out_ref, gain_ref, shift_ref, staged):
    tmpls, slab, pairs, _ = mine_ref.shape
    for half in range(2):
        total = sum(stat_ref[p] for p, (c, _) in enumerate(STAT_ORDER) if c == half)
        average = to_column(total, tmpls, 0) / count
        spread = to_column(total, tmpls, tmpls) / count - average * average
        gain_ref[pl.ds(half * tmpls, tmpls)] = 1.0 / jnp.sqrt(spread + SPREAD_FLOOR)
        shift_ref[pl.ds(half * tmpls, tmpls)] = average
    core = lax.axis_index(CORE)
    firsts = (core * tmpls, (1 - core) * tmpls)

    def tile(a, carry):
        for q in range(pairs // ROWS):
            best = total = None
            for first, ref in zip(firsts, (mine_ref, other_ref)):
                for group in range(tmpls // 4):
                    four = []
                    for t in range(4 * group, 4 * group + 4):
                        s = ref[t, a, pl.ds(q * ROWS, ROWS)]
                        g = gain_ref[pl.ds(first + t, ROWS, stride=0)]
                        m = shift_ref[pl.ds(first + t, ROWS, stride=0)]
                        four.append((s - m) * g)
                    part = (four[0] + four[1]) + (four[2] + four[3])
                    total = part if total is None else total + part
                    four = sort4(*four)
                    best = four if best is None else merge4(best, four)
            for r, value in enumerate((*best, total)):
                start = (q * ROWS * (TOP + 1) + r) * slab + a
                staged[pl.ds(start, ROWS, stride=(TOP + 1) * slab)] = value
        return carry

    lax.fori_loop(0, slab, tile, 0, unroll=4)
    size = (TOP + 1) * slab
    for place, chip in enumerate(CHIP_ORDER):
        out_ref[place * size : (place + 1) * size] = staged[chip * size : (chip + 1) * size]


def final_kernel(norm, in_ref, best_ref, sum_ref):
    peers = in_ref.shape[0]
    points = best_ref.shape[-1]
    fours = [tuple(in_ref[p, r] for r in range(TOP)) for p in range(peers)]
    total = in_ref[0, TOP]
    for p in range(1, peers):
        total = total + in_ref[p, TOP]
    while len(fours) > 1:
        fours = [merge4(u, v) for u, v in zip(fours[::2], fours[1::2])]
    total = total / norm
    for h in range(2):
        lanes = slice(h * points, (h + 1) * points)
        for r in range(TOP):
            best_ref[r, :, h, :] = fours[0][r][:, lanes]
        sum_ref[:, h, :] = total[:, lanes]


def body(spectrum):
    tmpls, slab, beta, doubled = spectrum.shape
    points = doubled // 2
    pairs = beta // 4
    chips = lax.axis_size(XY)
    peers = 2 * lax.axis_size("grid")
    vmem = pl.BlockSpec(memory_space=pltpu.VMEM)
    part = jax.ShapeDtypeStruct((tmpls, slab, pairs, LANES), jnp.float32)
    mine, send, stat = pl.pallas_call(
        score_kernel,
        out_shape=(part, part, jax.ShapeDtypeStruct((peers, 1, LANES), jnp.float32)),
        in_specs=[pl.BlockSpec(memory_space=pltpu.HBM)] * 2,
        out_specs=(vmem, vmem, vmem),
        scratch_shapes=[
            pltpu.VMEM(spectrum.shape, jnp.float32),
            pltpu.VMEM((2 * doubled, 2 * doubled), jnp.bfloat16),
            pltpu.VMEM((tmpls, ROWS, LANES), jnp.float32),
            pltpu.VMEM((tmpls, ROWS, LANES), jnp.float32),
            pltpu.SemaphoreType.DMA((len(CHUNKS),)),
            pltpu.SemaphoreType.DMA,
        ],
        compiler_params=pltpu.CompilerParams(vmem_limit_bytes=40 * 2**20),
        name="scores",
    )(*(
        pltpu.with_memory_space_constraint(a, pltpu.HBM)
        for a in (spectrum, jnp.asarray(split_table(points)))
    ))
    meeting = [[c * lax.axis_size("grid") + z for c, z in STAT_ORDER]]
    stats = lax.all_to_all(
        stat, (CORE, "grid"), split_axis=0, concat_axis=0, axis_index_groups=meeting, tiled=True
    )
    other = lax.ppermute(send, CORE, [(0, 1), (1, 0)])
    packed = pl.pallas_call(
        functools.partial(top_kernel, float(points**3)),
        out_shape=jax.ShapeDtypeStruct((chips * (TOP + 1) * slab, LANES), jnp.float32),
        in_specs=[vmem, vmem, vmem],
        out_specs=vmem,
        scratch_shapes=[
            pltpu.VMEM((2 * tmpls, LANES), jnp.float32),
            pltpu.VMEM((2 * tmpls, LANES), jnp.float32),
            pltpu.VMEM((chips * (TOP + 1) * slab, LANES), jnp.float32),
        ],
        compiler_params=pltpu.CompilerParams(vmem_limit_bytes=20 * 2**20),
        name="tops",
    )(mine, other, stats)
    packed = packed.reshape(chips, TOP + 1, slab, LANES)
    received = lax.all_to_all(
        packed, XY, split_axis=0, concat_axis=0, axis_index_groups=[list(CHIP_ORDER)], tiled=True
    )
    return pl.pallas_call(
        functools.partial(final_kernel, math.sqrt(2 * chips * tmpls)),
        out_shape=(
            jax.ShapeDtypeStruct((TOP, slab, 2, points), jnp.float32),
            jax.ShapeDtypeStruct((slab, 2, points), jnp.float32),
        ),
        in_specs=[vmem],
        out_specs=(vmem, vmem),
        compiler_params=pltpu.CompilerParams(vmem_limit_bytes=8 * 2**20),
        name="finish",
    )(received)


def solution(mesh):
    finer = Mesh(
        mesh.devices.reshape(4, 4, 2, mesh.shape["grid"]), (*XY, CORE, "grid")
    )
    tmpl = (*XY, CORE)
    return jax.shard_map(
        body,
        mesh=finer,
        in_specs=(P(tmpl, "grid", None, None),),
        out_specs=(P(None, "grid", tmpl, None), P("grid", tmpl, None)),
        check_vma=False,
    )
```

```python
import functools
import math

import jax
import jax.numpy as jnp
import numpy as np
from jax import lax
from jax.experimental import pallas as pl
from jax.experimental.pallas import tpu as pltpu
from jax.sharding import Mesh
from jax.sharding import PartitionSpec as P

TOP = 4
SPREAD_FLOOR = 0.25
ROWS = 8
LANES = 128
CHUNKS = (2, 2, 4, 8, 8, 8)
AHEAD = {0: 5, 1: 6}
FIRST = 4
LIVE = 4
STAT_ORDER = [(c, z) for c in (1, 0) for z in (4, 5, 6, 7, 0, 1, 2, 3)]
CHIP_ORDER = (10, 15, 14, 11, 9, 6, 13, 7, 12, 8, 5, 3, 2, 4, 1, 0)
XY = ("tmpl_0", "tmpl_1")
CORE = "tmpl_2"


def split_table(points):
    order = np.arange(points)
    angle = (order[:, None] * order[None, :] % points) * (2.0 * math.pi / points)
    table = np.concatenate([np.cos(angle), -np.sin(angle)], axis=0)
    mirror = (points - order) % points
    table[:points] = 0.5 * (table[:points] + table[:points][mirror])
    table[points:] = 0.5 * (table[points:] - table[points:][mirror])
    high = table.astype(jnp.bfloat16)
    low = (table - high.astype(np.float64)).astype(jnp.bfloat16)
    pair = [np.kron(np.eye(2), part.astype(np.float64)) for part in (high, low)]
    return np.concatenate(pair, axis=1).astype(jnp.bfloat16)


def diagonal(count, first):
    sub = lax.broadcasted_iota(jnp.int32, (count, LANES), 0)
    lane = lax.broadcasted_iota(jnp.int32, (count, LANES), 1)
    return lane == sub + first


def to_row(column, first):
    return jnp.sum(jnp.where(diagonal(column.shape[0], first), column, 0.0), axis=0, keepdims=True)


def to_column(row, count, first):
    kept = jnp.sum(jnp.where(diagonal(count, first), row, 0.0), axis=1, keepdims=True)
    return jnp.broadcast_to(kept, (count, LANES))


def score_kernel(
    x_hbm, w_hbm, mine_ref, send_ref, stat_ref, x_vmem, w_vmem, plain, square, sems, w_sem
):
    _, slab, beta, doubled = x_vmem.shape
    tmpls = mine_ref.shape[0]
    pairs = beta // 4
    rows = slab * pairs
    core = lax.axis_index(CORE)
    parities = (core, 1 - core)
    outs = (mine_ref, send_ref)

    edges = [sum(CHUNKS[:c]) for c in range(len(CHUNKS) + 1)]
    started = [0]

    def fetch(c):
        block = pl.ds(edges[c], CHUNKS[c])
        return pltpu.make_async_copy(x_hbm.at[block], x_vmem.at[block], sems.at[c])

    def fetch_up_to(c):
        for ahead in range(started[0], c):
            fetch(ahead).start()
        started[0] = max(started[0], c)

    table = pltpu.make_async_copy(w_hbm, w_vmem, w_sem)
    table.start()
    fetch_up_to(FIRST)
    table.wait()

    def parts(t, parity):
        sides = [
            x_vmem[t, :, pl.ds(2 * parity + h, pairs, stride=4), :].reshape(rows, doubled)
            for h in range(2)
        ]
        x = jnp.concatenate(sides, axis=1)
        high = x.astype(jnp.bfloat16)
        rest = x - high.astype(jnp.float32)
        mid = rest.astype(jnp.bfloat16)
        low = (rest - mid.astype(jnp.float32)).astype(jnp.bfloat16)
        return low, mid, high

    def run(*accs):
        first, accs = accs[:2], accs[2:]
        for m in range(2):
            pltpu.matmul_push_rhs(w_vmem[...], staging_register=0, mxu_index=m)
            zeros = jnp.zeros((16, 2 * doubled), jnp.bfloat16)
            pltpu.matmul_acc_lhs(first[m], zeros, load_staged_rhs=0)
            pltpu.matmul_pop(first[m])

        def take(t, u):
            plain_t = square_t = None
            for m in range(2):
                both = pltpu.matmul_pop(accs[2 * u + m])
                s = both[:, :LANES] + both[:, LANES:]
                outs[m][t] = s.reshape(slab, pairs, LANES)
                p = jnp.sum(s.reshape(-1, ROWS, LANES), axis=0)
                q = jnp.sum((s * s).reshape(-1, ROWS, LANES), axis=0)
                plain_t = p if plain_t is None else plain_t + p
                square_t = q if square_t is None else square_t + q
            plain[t] = plain_t
            square[t] = square_t

        for t in range(tmpls):
            if t in edges:
                c = edges.index(t)
                fetch(c).wait()
                fetch_up_to(AHEAD.get(c, 0))
            for m in range(2):
                for part in parts(t, parities[m]):
                    pltpu.matmul_acc_lhs(accs[2 * (t % LIVE) + m], part)
            if t:
                take(t - 1, (t - 1) % LIVE)
        take(tmpls - 1, (tmpls - 1) % LIVE)

    pl.run_scoped(
        run,
        *(pltpu.ACC(m)((16, 256), jnp.float32) for m in range(2)),
        *(pltpu.ACC(m)((rows, 256), jnp.float32) for _ in range(LIVE) for m in range(2)),
    )
    row = 0.0
    for i, part in enumerate((plain, square)):
        whole = jnp.sum(part[...], axis=1)
        row = row + to_row(jnp.sum(whole, axis=1, keepdims=True), i * tmpls)
    stat_ref[...] = jnp.broadcast_to(row[None], stat_ref.shape)


def order(a, b):
    return jnp.maximum(a, b), jnp.minimum(a, b)


def sort4(a, b, c, d):
    a, b = order(a, b)
    c, d = order(c, d)
    a, c = order(a, c)
    b, d = order(b, d)
    b, c = order(b, c)
    return a, b, c, d


def merge4(u, v):
    a, b, c, d = (jnp.maximum(u[i], v[3 - i]) for i in range(4))
    a, c = order(a, c)
    b, d = order(b, d)
    a, b = order(a, b)
    c, d = order(c, d)
    return a, b, c, d


def top_kernel(count, mine_ref, other_ref, stat_ref, out_ref, gain_ref, shift_ref, staged):
    tmpls, slab, pairs, _ = mine_ref.shape
    for half in range(2):
        total = sum(stat_ref[p] for p, (c, _) in enumerate(STAT_ORDER) if c == half)
        average = to_column(total, tmpls, 0) / count
        spread = to_column(total, tmpls, tmpls) / count - average * average
        gain_ref[pl.ds(half * tmpls, tmpls)] = 1.0 / jnp.sqrt(spread + SPREAD_FLOOR)
        shift_ref[pl.ds(half * tmpls, tmpls)] = average
    core = lax.axis_index(CORE)
    firsts = (core * tmpls, (1 - core) * tmpls)

    def tile(a, carry):
        for q in range(pairs // ROWS):
            best = total = None
            for first, ref in zip(firsts, (mine_ref, other_ref)):
                for group in range(tmpls // 4):
                    four = []
                    for t in range(4 * group, 4 * group + 4):
                        s = ref[t, a, pl.ds(q * ROWS, ROWS)]
                        g = gain_ref[pl.ds(first + t, ROWS, stride=0)]
                        m = shift_ref[pl.ds(first + t, ROWS, stride=0)]
                        four.append((s - m) * g)
                    part = (four[0] + four[1]) + (four[2] + four[3])
                    total = part if total is None else total + part
                    four = sort4(*four)
                    best = four if best is None else merge4(best, four)
            for r, value in enumerate((*best, total)):
                start = (q * ROWS * (TOP + 1) + r) * slab + a
                staged[pl.ds(start, ROWS, stride=(TOP + 1) * slab)] = value
        return carry

    lax.fori_loop(0, slab, tile, 0, unroll=4)
    size = (TOP + 1) * slab
    for place, chip in enumerate(CHIP_ORDER):
        out_ref[place * size : (place + 1) * size] = staged[chip * size : (chip + 1) * size]


def final_kernel(norm, in_ref, best_ref, sum_ref):
    peers = in_ref.shape[0]
    points = best_ref.shape[-1]
    fours = [tuple(in_ref[p, r] for r in range(TOP)) for p in range(peers)]
    total = in_ref[0, TOP]
    for p in range(1, peers):
        total = total + in_ref[p, TOP]
    while len(fours) > 1:
        fours = [merge4(u, v) for u, v in zip(fours[::2], fours[1::2])]
    total = total / norm
    for h in range(2):
        lanes = slice(h * points, (h + 1) * points)
        for r in range(TOP):
            best_ref[r, :, h, :] = fours[0][r][:, lanes]
        sum_ref[:, h, :] = total[:, lanes]


def body(spectrum):
    tmpls, slab, beta, doubled = spectrum.shape
    points = doubled // 2
    pairs = beta // 4
    chips = lax.axis_size(XY)
    peers = 2 * lax.axis_size("grid")
    vmem = pl.BlockSpec(memory_space=pltpu.VMEM)
    part = jax.ShapeDtypeStruct((tmpls, slab, pairs, LANES), jnp.float32)
    mine, send, stat = pl.pallas_call(
        score_kernel,
        out_shape=(part, part, jax.ShapeDtypeStruct((peers, 1, LANES), jnp.float32)),
        in_specs=[pl.BlockSpec(memory_space=pltpu.HBM)] * 2,
        out_specs=(vmem, vmem, vmem),
        scratch_shapes=[
            pltpu.VMEM((tmpls + 1, *spectrum.shape[1:]), jnp.float32),
            pltpu.VMEM((2 * doubled, 2 * doubled), jnp.bfloat16),
            pltpu.VMEM((tmpls, ROWS, LANES), jnp.float32),
            pltpu.VMEM((tmpls, ROWS, LANES), jnp.float32),
            pltpu.SemaphoreType.DMA((len(CHUNKS),)),
            pltpu.SemaphoreType.DMA,
        ],
        compiler_params=pltpu.CompilerParams(vmem_limit_bytes=40 * 2**20),
        name="scores",
    )(*(
        pltpu.with_memory_space_constraint(a, pltpu.HBM)
        for a in (spectrum, jnp.asarray(split_table(points)))
    ))
    meeting = [[c * lax.axis_size("grid") + z for c, z in STAT_ORDER]]
    stats = lax.all_to_all(
        stat, (CORE, "grid"), split_axis=0, concat_axis=0, axis_index_groups=meeting, tiled=True
    )
    other = lax.ppermute(send, CORE, [(0, 1), (1, 0)])
    packed = pl.pallas_call(
        functools.partial(top_kernel, float(points**3)),
        out_shape=jax.ShapeDtypeStruct((chips * (TOP + 1) * slab, LANES), jnp.float32),
        in_specs=[vmem, vmem, vmem],
        out_specs=vmem,
        scratch_shapes=[
            pltpu.VMEM((2 * tmpls + ROWS, LANES), jnp.float32),
            pltpu.VMEM((2 * tmpls + ROWS, LANES), jnp.float32),
            pltpu.VMEM(((chips + 1) * (TOP + 1) * slab, LANES), jnp.float32),
        ],
        compiler_params=pltpu.CompilerParams(vmem_limit_bytes=20 * 2**20),
        name="tops",
    )(mine, other, stats)
    packed = packed.reshape(chips, TOP + 1, slab, LANES)
    received = lax.all_to_all(
        packed, XY, split_axis=0, concat_axis=0, axis_index_groups=[list(CHIP_ORDER)], tiled=True
    )
    return pl.pallas_call(
        functools.partial(final_kernel, math.sqrt(2 * chips * tmpls)),
        out_shape=(
            jax.ShapeDtypeStruct((TOP, slab, 2, points), jnp.float32),
            jax.ShapeDtypeStruct((slab, 2, points), jnp.float32),
        ),
        in_specs=[vmem],
        out_specs=(vmem, vmem),
        compiler_params=pltpu.CompilerParams(vmem_limit_bytes=8 * 2**20),
        name="finish",
    )(received)


def solution(mesh):
    finer = Mesh(
        mesh.devices.reshape(4, 4, 2, mesh.shape["grid"]), (*XY, CORE, "grid")
    )
    tmpl = (*XY, CORE)
    return jax.shard_map(
        body,
        mesh=finer,
        in_specs=(P(tmpl, "grid", None, None),),
        out_specs=(P(None, "grid", tmpl, None), P("grid", tmpl, None)),
        check_vma=False,
    )
```
